128 devices in a mesh: dp: 16 (over z, y), tp: 8 (over x, core).
Axes of the slice: x: 4, y: 4, z: 4, core: 2. Of those that a mesh axis runs over, the one named last changes fastest.
Arguments:
- q_latent: bfloat16 [2048, 4, 1536], P('dp'), may hold values from -6 to 6
- new_latent: bfloat16 [2048, 4, 512], P('dp'), may hold values from -6 to 6
- new_rope: bfloat16 [2048, 4, 64], P('dp'), may hold values from -6 to 6
- cache_latent: bfloat16 [2048, 256, 512], P('dp'), may hold values from -6 to 6
- cache_rope: bfloat16 [2048, 64, 256], P('dp'), may hold values from -1200 to 1200
- lengths: int32 [2048], P('dp'), may hold values from 1 to 256
- assignment: int32 [16, 128], P('dp'), may hold values from 0 to 127, each once within a row
- w_uq: float32 [1536, 12288], P(('dp', 'tp')), may hold values from -0.15625 to 0.15625
- w_uk: float32 [512, 8192], P(('dp', 'tp')), may hold values from -3 to 3
- w_uv: float32 [512, 8192], P(('dp', 'tp')), may hold values from -0.25 to 0.25
- w_o: float32 [8192, 7168], P(None, ('dp', 'tp')), may hold values from -0.0625 to 0.0625
Outputs:
- attention_out: bfloat16 [2048, 4, 7168], P('dp', None, 'tp')
- weight_norm: float32 [1], replicated
The draws below stay inside these ranges and needn't reach their ends.
Inputs may be any that keep to these rules, and one draw needn't show every extreme that they name: Each row of assignment is a permutation of 0 to 127.
All inputs are finite; a program needn't handle non-finite values.
Results may differ from the reference program's by a relative error of at most 0.006.
The reference program's roundings to bfloat16 on the way count: a program that leaves them out, or rounds other values in their place, can miss the bound.
Values may be sent and summed in bfloat16 or wider, within the bound.
A program may use at most 256 MiB of HBM per device.

```python
import jax
import jax.numpy as jnp
from jax import lax

D = 7168
QRANK = 1536
KVRANK = 512
NOPE = 128
ROPE = 64
VDIM = 128
HEADS = 64
NEWTOK = 4
SEQ_REP = 128
CACHE = 256
REPLICAS = 16
SEQS = 2048


def draw_cache_rope(key, part):
    values = jnp.clip(jax.random.normal(key, (SEQS, ROPE, CACHE), jnp.float32), -4.0, 4.0)
    return values.astype(jnp.bfloat16)


def place_ends(entries, stream_key, least, top_value):
    spot = [jax.random.randint(jax.random.fold_in(stream_key, axis), (), 0, length) for axis, length in enumerate(entries.shape)]
    longest = entries.shape.index(max(entries.shape))
    next_to = spot[:longest] + [(spot[longest] + 1) % entries.shape[longest]] + spot[longest + 1:]
    return entries.at[tuple(spot)].set(least).at[tuple(next_to)].set(top_value)


def strengthened(entries, rng, source, target, shards_of, factor):
    owner, partner = [(jnp.arange(entries.shape[position]) // (entries.shape[position] // shards_of)).reshape([-1 if axis == position else 1 for axis in range(entries.ndim)]) for position in (source, target)]
    chosen = jax.random.permutation(rng, shards_of)[partner]
    strong = (owner == chosen) | (owner == (partner + shards_of // 2) % shards_of)
    return jnp.where(strong, factor * entries, entries)


def level_of(rng, dims, cuts, smallest, top_value):
    gain, own = 1.0, jax.random.fold_in(rng, 6)
    for axis_at, shards_of in cuts:
        heights = jnp.exp(jax.random.uniform(jax.random.fold_in(own, axis_at), (shards_of,), jnp.float32, smallest / len(cuts), top_value / len(cuts)))
        gain = gain * jnp.repeat(heights, dims[axis_at] // shards_of).reshape([-1 if axis == axis_at else 1 for axis in range(len(dims))])
    return gain


def noise(stream_key, extent, width, reach, pieces=(), held_as=jnp.bfloat16):
    entries = jax.random.normal(stream_key, extent, jnp.float32) * width
    if len(pieces) > 0:
        entries = level_of(stream_key, extent, pieces, -0.22, 0.18) * entries
    return jnp.clip(entries, min=-reach, max=reach).astype(held_as)


def heavy_noise(own_key, shape, deviation, bound, split, heavy, held_as=jnp.bfloat16):
    entries = deviation * jax.random.normal(own_key, shape, jnp.float32)
    if split:
        entries = entries * level_of(own_key, shape, split, -0.22, 0.18)
    return jnp.clip(strengthened(entries, jax.random.fold_in(own_key, 3), *heavy), -bound, bound).astype(held_as)


def setup_inputs(seed: int = 0) -> dict:
    arg_keys = jax.random.split(jax.random.key(seed), 12)
    return {
        "q_latent": noise(arg_keys[0], (SEQS, NEWTOK, QRANK), 1.0, 6.0, ((0, 16),)),
        "new_latent": noise(arg_keys[1], (SEQS, NEWTOK, KVRANK), 1.0, 6.0, ((0, 16),)),
        "new_rope": noise(arg_keys[2], (SEQS, NEWTOK, ROPE), 1.0, 6.0, ((0, 16),)),
        "cache_latent": noise(arg_keys[3], (SEQS, CACHE, KVRANK), 1.0, 6.0, ((0, 16),)),
        "cache_rope": draw_cache_rope(jax.random.fold_in(arg_keys[11], 71), 0),
        "lengths": place_ends(jax.random.randint(arg_keys[5], (SEQS,), 1, CACHE + 1), jax.random.fold_in(arg_keys[5], 1), 1, CACHE).astype(jnp.int32),
        "assignment": jax.vmap(lambda own: jax.random.permutation(own, SEQ_REP))(jax.random.split(arg_keys[6], REPLICAS)).reshape((REPLICAS, SEQ_REP)).astype(jnp.int32),
        "w_uq": noise(arg_keys[7], (QRANK, HEADS * (NOPE + ROPE)), QRANK ** -0.5, 0.15625, ((0, 128),), jnp.float32),
        "w_uk": heavy_noise(arg_keys[8], (KVRANK, HEADS * NOPE), 0.125, 3.0, ((0, 128),), (0, 1, 128, 5.5), jnp.float32),
        "w_uv": noise(arg_keys[9], (KVRANK, HEADS * VDIM), KVRANK ** -0.5, 0.25, ((0, 128),), jnp.float32),
        "w_o": noise(arg_keys[10], (HEADS * VDIM, D), (HEADS * VDIM) ** -0.5, 0.0625, ((1, 128),), jnp.float32),
    }


def widen(values):
    return lax.optimization_barrier(values).astype(jnp.float32)

def rotate_half(values, positions):
    half_width = values.shape[-1] // 2
    frequency = 10000.0 ** (-jnp.arange(half_width, dtype=jnp.float32) / half_width)
    angles = positions.astype(jnp.float32)[:, :, None, None] * frequency
    cosine = jnp.cos(angles)
    sine_part = jnp.sin(angles)
    lower_half = values[..., :half_width]
    upper_half = values[..., half_width:]
    return jnp.concatenate([lower_half * cosine - upper_half * sine_part, upper_half * cosine + lower_half * sine_part], axis=-1)

def reference(q_latent, new_latent, new_rope, cache_latent, cache_rope, lengths, assignment, w_uq, w_uk, w_uv, w_o):
    high = lax.Precision.HIGHEST
    squares_total = jnp.sum(w_uq * w_uq) + jnp.sum(w_uk * w_uk) + jnp.sum(w_uv * w_uv) + jnp.sum(w_o * w_o)
    weight_norm = jnp.sqrt(squares_total / (HEADS * (NOPE + ROPE) + 2 * HEADS * NOPE + D)).reshape(1)
    query_up = w_uq.astype(jnp.bfloat16)
    key_up = widen(w_uk.astype(jnp.bfloat16)).reshape(KVRANK, HEADS, NOPE)
    value_up = widen(w_uv.astype(jnp.bfloat16)).reshape(KVRANK, HEADS, VDIM)
    out_proj = w_o.astype(jnp.bfloat16)
    scale = (NOPE + ROPE) ** (-0.5)

    def replica(inputs):
        queries, latents, ropes, cache_lat, cache_rot, lens, order = inputs
        slot_lat = widen(cache_lat[order])
        slot_rot = widen(cache_rot[order])
        slot_len = lens[order]
        projected = jnp.dot(queries.reshape(SEQ_REP * NEWTOK, QRANK), query_up, preferred_element_type=jnp.float32)
        projected = projected.astype(jnp.bfloat16).reshape(SEQ_REP, NEWTOK, HEADS, NOPE + ROPE)
        query_nope = widen(projected[..., :NOPE])
        positions = slot_len[:, None] + jnp.arange(NEWTOK, dtype=jnp.int32)[None, :]
        query_rot = widen(rotate_half(widen(projected[..., NOPE:]), positions).astype(jnp.bfloat16))
        absorbed = jnp.einsum('sqhn,chn->sqhc', query_nope, key_up, precision=high).astype(jnp.bfloat16)
        absorbed = widen(absorbed)
        new_lat = widen(latents)
        new_rot = widen(ropes)
        cache_scores = (jnp.einsum('sqhc,stc->sqht', absorbed, slot_lat, precision=high) + jnp.einsum('sqhr,srt->sqht', query_rot, slot_rot, precision=high)) * scale
        valid = jnp.arange(CACHE, dtype=jnp.int32)[None, :] < slot_len[:, None]
        cache_scores = jnp.where(valid[:, None, None, :], cache_scores, -jnp.inf)
        new_scores = (jnp.einsum('sqhc,skc->sqhk', absorbed, new_lat, precision=high) + jnp.einsum('sqhr,skr->sqhk', query_rot, new_rot, precision=high)) * scale
        causal = jnp.arange(NEWTOK)[:, None] >= jnp.arange(NEWTOK)[None, :]
        new_scores = jnp.where(causal[None, :, None, :], new_scores, -jnp.inf)
        scores = jnp.concatenate([cache_scores, new_scores], axis=-1)
        largest = lax.optimization_barrier(jnp.max(scores, axis=-1, keepdims=True))
        expo = jnp.exp(scores - largest)
        weights = widen((expo / lax.optimization_barrier(jnp.sum(expo, axis=-1, keepdims=True))).astype(jnp.bfloat16))
        latent_out = jnp.einsum('sqht,stc->sqhc', weights[..., :CACHE], slot_lat, precision=high) + jnp.einsum('sqhk,skc->sqhc', weights[..., CACHE:], new_lat, precision=high)
        latent_out = widen(latent_out.astype(jnp.bfloat16))
        head_out = jnp.einsum('sqhc,chv->sqhv', latent_out, value_up, precision=high).astype(jnp.bfloat16)
        result = jnp.dot(head_out.reshape(SEQ_REP * NEWTOK, HEADS * VDIM), out_proj, preferred_element_type=jnp.float32)
        return result.astype(jnp.bfloat16).reshape(SEQ_REP, NEWTOK, D)
    outputs = lax.map(replica, (q_latent.reshape(REPLICAS, SEQ_REP, NEWTOK, QRANK), new_latent.reshape(REPLICAS, SEQ_REP, NEWTOK, KVRANK), new_rope.reshape(REPLICAS, SEQ_REP, NEWTOK, ROPE), cache_latent.reshape(REPLICAS, SEQ_REP, CACHE, KVRANK), cache_rope.reshape(REPLICAS, SEQ_REP, ROPE, CACHE), lengths.reshape(REPLICAS, SEQ_REP), assignment))
    return (outputs.reshape(SEQS, NEWTOK, D), weight_norm)
```

```python
import jax
import jax.numpy as jnp
from jax import lax
from jax.experimental import pallas as pl
from jax.experimental.pallas import tpu as pltpu
from jax.sharding import Mesh
from jax.sharding import PartitionSpec as P

D = 7168
QRANK = 1536
KVRANK = 512
NOPE = 128
ROPE = 64
VDIM = 128
HEADS = 64
NEWTOK = 4
CACHE = 256
SEQS = 128
TOK = SEQS * NEWTOK
HL = 8
GROUPS = SEQS // 4
SLOTS = 4
BF = jnp.bfloat16
F32 = jnp.float32
DP_TP = ("dp_0", "dp_1", "tp_0", "tp_1")
TP = ("tp_0", "tp_1")
DP = ("dp_0", "dp_1")
SCALE = (NOPE + ROPE) ** (-0.5)


def nt(a, b):
    return lax.dot_general(a, b, (((1,), (1,)), ((), ())), preferred_element_type=F32)


def nn(a, b):
    return lax.dot_general(a, b, (((1,), (0,)), ((), ())), preferred_element_type=F32)


def project(q_ref, u_ref, cos_ref, sin_ref, abs_ref, qr_ref):
    def nope_pair(i, carry):
        cols = pl.ds(pl.multiple_of(i * 256, 256), 256)
        both = nn(q_ref[...], u_ref[:, :, 0:96, cols].reshape(QRANK, 256)).astype(BF)
        for j in range(2):
            own_cols = pl.ds(pl.multiple_of(i * 256 + j * 128, 128), 128)
            keys = u_ref[:, :, 96:128, own_cols].reshape(KVRANK, 128)
            abs_ref[i * 2 + j] = nt(both[:, j * 128 : (j + 1) * 128], keys).astype(BF)
        return carry

    lax.fori_loop(0, 4, nope_pair, 0)
    lane = lax.broadcasted_iota(jnp.int32, (TOK, 128), 1)
    row = lax.broadcasted_iota(jnp.int32, (TOK, 128), 0)
    own = lax.rem(row // 4, 4)
    low = lax.rem(lane, 64) < 32

    def pe_quad(i, carry):
        cols = pl.ds(pl.multiple_of(1024 + i * 256, 256), 256)
        four = nn(q_ref[...], u_ref[:, :, 0:96, cols].reshape(QRANK, 256)).astype(BF).astype(F32)
        for j in range(2):
            pe = four[:, j * 128 : (j + 1) * 128]
            other = jnp.where(low, pltpu.roll(pe, 96, 1), pltpu.roll(pe, 32, 1))
            rot = pe * cos_ref[...] + other * sin_ref[...]
            flip = pltpu.roll(rot, 64, 1)
            for odd in range(2):
                twice = jnp.where((lane < 64) == (odd == 0), rot, flip)
                head = i * 4 + j * 2 + odd
                for half in range(2):
                    kept = jnp.where(own == 2 * half + lane // 64, twice, 0.0)
                    qr_ref[head, :, half * 128 : (half + 1) * 128] = kept.astype(BF)
        return carry

    lax.fori_loop(0, 2, pe_quad, 0)


def scores_of(g, abs_ref, qr_ref, latn_ref, ropn_ref, lat, rop, sc_ref, scn_ref):
    rows = pl.ds(pl.multiple_of(g * 16, 16), 16)
    q = abs_ref[:, rows, :].reshape(128, KVRANK)
    qr = qr_ref[:, rows, :].reshape(128, 256)
    seq = lax.rem(lax.broadcasted_iota(jnp.int32, (128, KVRANK), 0) // 4, 4)
    zero = jnp.zeros_like(q)
    parts = jnp.concatenate([jnp.where(seq == s, q, zero) for s in range(4)], axis=1)
    keys = jnp.concatenate([lat[s] for s in range(4)], axis=1)
    sc_ref[...] = nt(parts, keys) + nn(qr, rop[...].reshape(256, CACHE))
    scn_ref[...] = nt(q, latn_ref[rows, :]) + nt(qr, ropn_ref[rows, :])


def attend(g, len_ref, latn_ref, lat, sc_ref, scn_ref, lo_ref):
    row = lax.broadcasted_iota(jnp.int32, (128, CACHE), 0)
    seq = lax.rem(row // 4, 4)
    limit = jnp.where(
        seq == 0,
        len_ref[g * 4],
        jnp.where(
            seq == 1, len_ref[g * 4 + 1], jnp.where(seq == 2, len_ref[g * 4 + 2], len_ref[g * 4 + 3])
        ),
    )
    at = lax.broadcasted_iota(jnp.int32, (128, CACHE), 1)
    sc = jnp.where(at < limit, sc_ref[...] * SCALE, -jnp.inf)
    nrow = lax.broadcasted_iota(jnp.int32, (128, 16), 0)
    ncol = lax.broadcasted_iota(jnp.int32, (128, 16), 1)
    fits = (lax.rem(nrow // 4, 4) == ncol // 4) & (lax.rem(ncol, 4) <= lax.rem(nrow, 4))
    scn = jnp.where(fits, scn_ref[...] * SCALE, -jnp.inf)
    top = jnp.maximum(
        jnp.max(sc, axis=1, keepdims=True), jnp.max(scn, axis=1, keepdims=True)
    )
    ex = jnp.exp(sc - top)
    exn = jnp.exp(scn - top)
    total = jnp.sum(ex, axis=1, keepdims=True) + jnp.sum(exn, axis=1, keepdims=True)
    share = 1.0 / total
    w = (ex * share).astype(BF)
    wn = (exn * share).astype(BF)
    zero = jnp.zeros_like(w)
    parts = jnp.concatenate([jnp.where(seq == s, w, zero) for s in range(4)], axis=1)
    rows = pl.ds(pl.multiple_of(g * 16, 16), 16)
    out = nn(parts, lat[...].reshape(4 * CACHE, KVRANK)) + nn(wn, latn_ref[rows, :])
    lo_ref[:, rows, :] = out.astype(BF).reshape(HL, 16, KVRANK)


MESH = pl.DeviceIdType.MESH
CHUNKS = 4
HALF = 64


def around(i, d):
    return lax.rem(i + d + 4, 4)


def layer_kernel(
    uq_ref, wk_ref, wv_ref, wo_ref, q_ref, latk_ref, ropk_ref, selk_ref, sel_ref, cos_ref, sin_ref,
    len_ref, lat_hbm, rop_hbm,
    out_ref, norm_ref,
    stage, packs, rp, opack, orp, u_ref, wo_all, nsend, ntp, ny, nz,
    qs_ref, latn_ref, ropn_ref, abs_ref, qr_ref, lo_ref, lat_ref, rop_ref, sc0, scn0, sc1, scn1,
    ho_ref, hb_ref, ct_ref, r1_ref, rx_ref, fs_ref, ft_ref, ot_ref,
    lat_sem, rop_sem, a2a_s, a2a_r, o2a_s, o2a_r, nt_s, nt_r, nyz_s, nyz_r, ag_s, ag_r,
    oz_s, oz_r, od_s, od_r, d2_s, d2_r, hy_s, hy_r, r1_s, r1_r, r2_s, r2_r, f_s, f_r,
):
    z, y = lax.axis_index("dp_0"), lax.axis_index("dp_1")
    x, c = lax.axis_index("tp_0"), lax.axis_index("tp_1")
    t = x * 2 + c
    sends = []

    def copy_to(src, dst, ss, rs, **axes):
        names = {"z": "dp_0", "y": "dp_1", "x": "tp_0", "c": "tp_1"}
        return pltpu.make_async_remote_copy(
            src_ref=src, dst_ref=dst, send_sem=ss, recv_sem=rs,
            device_id={names[n]: v for n, v in axes.items()}, device_id_type=MESH,
        )

    def send(src, dst, ss, rs, **axes):
        made = copy_to(src, dst, ss, rs, **axes)
        made.start()
        sends.append(made)

    def arrived(dst, ss, rs):
        copy_to(dst, dst, ss, rs, c=1 - c).wait_recv()

    barrier = pltpu.get_barrier_semaphore()

    def greet(**axes):
        names = {"z": "dp_0", "y": "dp_1", "x": "tp_0", "c": "tp_1"}
        pl.semaphore_signal(
            barrier, inc=1, device_id={names[n]: v for n, v in axes.items()}, device_id_type=MESH
        )

    for dt in range(1, 8):
        peer = lax.rem(t + dt, 8)
        greet(x=peer // 2, c=lax.rem(peer, 2))
    for d in range(1, 4):
        greet(z=around(z, d))
        greet(y=around(y, d))
        greet(y=around(y, d), c=1 - c)

    def fetch(g):
        slot = lax.rem(g, SLOTS)
        return (
            pltpu.make_async_copy(lat_hbm.at[pl.ds(g * 4, 4)], lat_ref.at[slot], lat_sem.at[slot]),
            pltpu.make_async_copy(rop_hbm.at[pl.ds(g * 4, 4)], rop_ref.at[slot], rop_sem.at[slot]),
        )

    def start(g):
        for made in fetch(g):
            made.start()

    def wait(g):
        for made in fetch(g):
            made.wait()

    for g in range(SLOTS - 1):
        start(g)

    lane12 = lax.broadcasted_iota(jnp.int32, (12, 128), 1)

    def fold(v):
        rows, cols = v.shape
        total = jnp.zeros((8, 128), F32)
        for i in range(rows // 8):
            for j in range(cols // 128):
                part = v[i * 8 : i * 8 + 8, j * 128 : j * 128 + 128]
                total = total + part * part
        return total

    def pack_one(p, squares):
        for i in range(4):
            v = uq_ref[:, pl.ds(pl.multiple_of(p * 1536 + i * 384, 128), 384)]
            v0, v1, v2 = v[:, 0:128], v[:, 128:256], v[:, 256:384]
            stage[p, 0:12, i * 256 : i * 256 + 128] = v0
            stage[p, 0:12, i * 256 + 128 : i * 256 + 256] = pltpu.roll(
                jnp.where(lane12 < 64, v2, v1), 64, 1
            )
            stage[p, 0:12, 1024 + i * 128 : 1152 + i * 128] = jnp.where(lane12 < 64, v1, v2)
            stage[p, i * 4 : i * 4 + 4, 1536:1792] = wv_ref[
                :, pl.ds(pl.multiple_of(p * 1024 + i * 256, 128), 256)
            ]
        stage[p, 12:16, 0:1024] = wk_ref[:, pl.ds(pl.multiple_of(p * 1024, 128), 1024)]
        stage[p, 12:16, 1024:1536] = jnp.zeros((4, 512), F32)
        whole = stage[p]
        packs[p] = whole.astype(BF)
        return squares + fold(whole)

    squares = lax.fori_loop(0, 8, pack_one, jnp.zeros((8, 128), F32))
    pl.semaphore_wait(barrier, 16)
    for dt in range(1, 8):
        peer = lax.rem(t + dt, 8)
        send(packs.at[peer], rp.at[t], a2a_s.at[dt], a2a_r.at[dt], x=peer // 2, c=lax.rem(peer, 2))
    rp[t] = packs[t]

    def pack_out(p, squares):
        v = wo_ref[:, pl.ds(pl.multiple_of(p * 1024, 128), 1024)]
        opack[p] = v.astype(BF)
        return squares + fold(v)

    squares = lax.fori_loop(0, 8, pack_out, squares)
    nsend[0] = squares
    ntp[t] = squares
    for dt in range(1, 8):
        peer = lax.rem(t + dt, 8)
        where = dict(x=peer // 2, c=lax.rem(peer, 2))
        send(nsend.at[0], ntp.at[t], nt_s.at[dt], nt_r.at[dt], **where)
        send(opack.at[peer], orp.at[t], o2a_s.at[dt], o2a_r.at[dt], **where)
    orp[t] = opack[t]

    for dt in range(1, 8):
        arrived(rp.at[lax.rem(t + 8 - dt, 8)], a2a_s.at[dt], a2a_r.at[dt])
    big = rp[...].reshape(128, 1792)
    r = lax.broadcasted_iota(jnp.int32, (128, 128), 0)
    col = lax.broadcasted_iota(jnp.int32, (128, 128), 1)
    origin = jnp.where(
        r < 96, (r // 12) * 16 + lax.rem(r, 12), ((r - 96) // 4) * 16 + 12 + lax.rem(r - 96, 4)
    )
    order = jnp.where(col == origin, 1.0, 0.0).astype(BF)
    sorted_rows = nn(order, big[:, 0:1536]).astype(BF)
    r32 = lax.broadcasted_iota(jnp.int32, (32, 128), 0)
    col32 = lax.broadcasted_iota(jnp.int32, (32, 128), 1)
    uv_parts = []
    for i in range(4):
        pick = jnp.where(col32 == (r32 // 4) * 16 + i * 4 + lax.rem(r32, 4), 1.0, 0.0).astype(BF)
        uv_parts.append(nn(pick, big[:, 1536:1792]).astype(BF))
    own_uv = jnp.concatenate(uv_parts, axis=1)
    u_ref[z, y, 0:96, 0:1536] = sorted_rows[0:96]
    u_ref[z, y, 96:128, 0:1024] = sorted_rows[96:128, 0:1024]
    u_ref[z, y, 96:128, 1024:1664] = own_uv[:, 0:640]
    for i in range(3):
        u_ref[z, y, i * 32 : i * 32 + 32, 1536:1664] = own_uv[:, 640 + i * 128 : 768 + i * 128]

    def piece(half, ia, ib, sub=None):
        rows = pl.ds(half * 64, 64) if sub is None else pl.ds(half * 64 + sub * 32, 32)
        return u_ref.at[ib, ia, rows] if half == 0 else u_ref.at[ia, ib, rows]

    def step(half, along_first, to):
        first, second = ("y", "z") if half == 0 else ("z", "y")
        return {first if along_first else second: to}

    where_a = [y, z]
    where_b = [z, y]

    def sems(half, n):
        return ag_s.at[half * 20 + n], ag_r.at[half * 20 + n]

    offsets = (0, -1, 1, 2)

    def second_send(half, p):
        a, b = where_a[half], where_b[half]
        ia = around(a, offsets[p])
        for k, d in enumerate((1, -1)):
            ref = piece(half, ia, b)
            send(ref, ref, *sems(half, 4 + p * 2 + k), **step(half, False, around(b, d)))

    def second_forward(half, p):
        a, b = where_a[half], where_b[half]
        ia = around(a, offsets[p])
        for k, d in enumerate((1, -1)):
            arrived(piece(half, ia, around(b, -d)), *sems(half, 4 + p * 2 + k))
            ref = piece(half, ia, around(b, -d), k)
            send(ref, ref, *sems(half, 12 + p * 2 + k), **step(half, False, around(b, d)))

    for half in range(2):
        a, b = where_a[half], where_b[half]
        for k, d in enumerate((1, -1)):
            ref = piece(half, a, b)
            send(ref, ref, *sems(half, k), **step(half, True, around(a, d)))
    for half in range(2):
        second_send(half, 0)

    qs_ref[...] = nn(selk_ref[...], q_ref[...]).astype(BF)
    latn_ref[...] = nn(selk_ref[...], latk_ref[...]).astype(BF)
    rope_rows = jnp.concatenate([ropk_ref[k] for k in range(4)], axis=1)
    ropn_ref[...] = nt(selk_ref[...], jnp.concatenate([rope_rows] * 4, axis=0)).astype(BF)

    for dt in range(1, 8):
        arrived(ntp.at[lax.rem(t + 8 - dt, 8)], nt_s.at[dt], nt_r.at[dt])
    line = ntp[0]
    for i in range(1, 8):
        line = line + ntp[i]
    nsend[1] = line
    ny[y] = line
    for d in range(1, 4):
        send(nsend.at[1], ny.at[y], nyz_s.at[0, d], nyz_r.at[0, d], y=around(y, d))

    for half in range(2):
        a, b = where_a[half], where_b[half]
        for k, d in enumerate((1, -1)):
            arrived(piece(half, around(a, -d), b), *sems(half, k))
            ref = piece(half, around(a, -d), b, k)
            send(ref, ref, *sems(half, 2 + k), **step(half, True, around(a, d)))
    for half in range(2):
        second_send(half, 1)
        second_send(half, 2)
    for half in range(2):
        second_forward(half, 0)
    for d in range(1, 4):
        arrived(ny.at[around(y, -d)], nyz_s.at[0, d], nyz_r.at[0, d])
    plane = ((ny[0] + ny[1]) + ny[2]) + ny[3]
    nsend[2] = plane
    nz[z] = plane
    for d in range(1, 4):
        send(nsend.at[2], nz.at[z], nyz_s.at[1, d], nyz_r.at[1, d], z=around(z, d))
    for half in range(2):
        a, b = where_a[half], where_b[half]
        for k in range(2):
            arrived(piece(half, around(a, 2), b, k), *sems(half, 2 + k))
        second_send(half, 3)
    for p in range(1, 3):
        for half in range(2):
            second_forward(half, p)

    for dt in range(1, 8):
        arrived(orp.at[lax.rem(t + 8 - dt, 8)], o2a_s.at[dt], o2a_r.at[dt])
    wo_all[c, z] = jnp.concatenate([orp[i].astype(F32) for i in range(8)], axis=0).astype(BF)
    for half in range(2):
        second_forward(half, 3)
    send(wo_all.at[c, z], wo_all.at[c, z], od_s.at[0], od_r.at[0], c=1 - c)
    for k, d in enumerate((1, -1)):
        send(wo_all.at[c, z], wo_all.at[c, z], oz_s.at[k], oz_r.at[k], z=around(z, d))
    for p in range(4):
        for half in range(2):
            a, b = where_a[half], where_b[half]
            for k in range(2):
                last = piece(half, around(a, offsets[p]), around(b, 2), k)
                arrived(last, *sems(half, 12 + p * 2 + k))
    for d in range(1, 4):
        arrived(nz.at[around(z, -d)], nyz_s.at[1, d], nyz_r.at[1, d])
    everything = ((nz[0] + nz[1]) + nz[2]) + nz[3]
    everything = jnp.sum(jnp.sum(everything, axis=1, keepdims=True), axis=0, keepdims=True)
    entries = HEADS * (NOPE + ROPE) + 2 * HEADS * NOPE + D
    norm_ref[...] = jnp.broadcast_to(jnp.sqrt(everything / entries), (8, 128))

    project(qs_ref, u_ref, cos_ref, sin_ref, abs_ref, qr_ref)

    def score(g, sc, scn):
        slot = lax.rem(g, SLOTS)
        scores_of(g, abs_ref, qr_ref, latn_ref, ropn_ref, lat_ref.at[slot], rop_ref.at[slot], sc, scn)

    def finish(g, sc, scn):
        attend(g, len_ref, latn_ref, lat_ref.at[lax.rem(g, SLOTS)], sc, scn, lo_ref)

    wait(0)
    score(0, sc0, scn0)

    def two(i, carry):
        g = i * 2

        @pl.when(g + 3 < GROUPS)
        def _():
            start(g + 3)

        wait(g + 1)
        score(g + 1, sc1, scn1)
        finish(g, sc0, scn0)

        @pl.when(g + 4 < GROUPS)
        def _():
            start(g + 4)

        @pl.when(g + 2 < GROUPS)
        def _():
            wait(g + 2)

        score(jnp.minimum(g + 2, GROUPS - 1), sc0, scn0)
        finish(g + 1, sc1, scn1)
        return carry

    def out_first():
        for k, d in enumerate((1, -1)):
            near = wo_all.at[c, around(z, -d)]
            arrived(near, oz_s.at[k], oz_r.at[k])
            part = wo_all.at[c, around(z, -d), pl.ds(k * 224, 224)]
            send(part, part, oz_s.at[2 + k], oz_r.at[2 + k], z=around(z, d))
            send(near, near, od_s.at[1 + k], od_r.at[1 + k], c=1 - c)

    def out_second():
        far = wo_all.at[c, around(z, 2)]
        for k in range(2):
            arrived(far.at[pl.ds(k * 224, 224)], oz_s.at[2 + k], oz_r.at[2 + k])
        send(far, far, od_s.at[3], od_r.at[3], c=1 - c)

    def out_ready():
        for n, d in enumerate((0, -1, 1, 2)):
            arrived(wo_all.at[1 - c, around(z, d)], od_s.at[n], od_r.at[n])

    def heads_done(j):
        rows = slice(j * 128, j * 128 + 128)
        for h in range(HL):
            if h < 5:
                up = u_ref[:, :, 96:128, 1024 + h * 128 : 1152 + h * 128].reshape(KVRANK, 128)
            else:
                up = u_ref[:, :, (h - 5) * 32 : (h - 4) * 32, 1536:1664].reshape(KVRANK, 128)
            both = nn(lo_ref[h, rows, :], up).astype(BF)
            for half in range(2):
                ho_ref[j, half, :, h * 128 : h * 128 + 128] = both[half * 64 : half * 64 + 64]
        hb_ref[j, y, c] = ho_ref[j, c]
        send(ho_ref.at[j, 1 - c], hb_ref.at[j, y, c], d2_s.at[j], d2_r.at[j], c=1 - c)
        for k, d in enumerate((1, -1)):
            send(
                ho_ref.at[j, c], hb_ref.at[j, y, c], hy_s.at[j, k], hy_r.at[j, k], y=around(y, d)
            )

    def partner_half(j):
        ref = hb_ref.at[j, y, 1 - c]
        arrived(ref, d2_s.at[j], d2_r.at[j])
        for k, d in enumerate((1, -1)):
            send(ref, ref, hy_s.at[j, 2 + k], hy_r.at[j, 2 + k], y=around(y, d))

    def pass_on(j):
        for k, d in enumerate((1, -1)):
            arrived(hb_ref.at[j, around(y, -d), c], hy_s.at[j, k], hy_r.at[j, k])
            arrived(hb_ref.at[j, around(y, -d), 1 - c], hy_s.at[j, 2 + k], hy_r.at[j, 2 + k])
            ref = hb_ref.at[j, around(y, -d), k]
            send(ref, ref, hy_s.at[j, 4 + k], hy_r.at[j, 4 + k], y=around(y, d))

    def multiply(j):
        for k in range(2):
            arrived(hb_ref.at[j, around(y, 2), k], hy_s.at[j, 4 + k], hy_r.at[j, 4 + k])

        def block(n):
            zs = lax.rem(x + n, 4)
            tokens = jnp.concatenate(
                [hb_ref[j, :, k].reshape(4 * HALF, 1024) for k in range(2)], axis=1
            )
            columns = jnp.concatenate([wo_all[k, zs] for k in range(2)], axis=1)
            ct_ref[j, zs] = nt(columns, tokens).astype(BF)

        block(2)
        for k, d in enumerate((1, -1)):
            send(
                ct_ref.at[j, around(x, 2), pl.ds(k * 224, 224)], r1_ref.at[j, k],
                r1_s.at[j, k], r1_r.at[j, k], x=around(x, d),
            )

        def rest(n, carry):
            block(jnp.where(n == 0, 1, jnp.where(n == 1, 3, 0)))
            return carry

        lax.fori_loop(0, 3, rest, 0)

    def add_far(j):
        for k, d in enumerate((1, -1)):
            arrived(r1_ref.at[j, k], r1_s.at[j, k], r1_r.at[j, k])
            rows = slice(k * 224, k * 224 + 224)
            near = around(x, d)
            both = ct_ref[j, near, rows].astype(F32) + r1_ref[j, k].astype(F32)
            ct_ref[j, near, rows] = both.astype(BF)
            send(ct_ref.at[j, near], rx_ref.at[j, k], r2_s.at[j, k], r2_r.at[j, k], x=near)

    returns = []

    def add_near(j):
        for k in range(2):
            arrived(rx_ref.at[j, k], r2_s.at[j, k], r2_r.at[j, k])
        fs_ref[j % 2] = (
            ct_ref[j, x].astype(F32) + rx_ref[j, 0].astype(F32) + rx_ref[j, 1].astype(F32)
        )
        if j % 2 == 0:
            return
        pair = j // 2
        lane = lax.broadcasted_iota(jnp.int32, (448, 128), 1)
        for v in range(2):
            early = fs_ref[0, :, v * 128 : v * 128 + 128]
            late = fs_ref[1, :, v * 128 : v * 128 + 128]
            ft_ref[pair, 2 * v] = jnp.where(lane < 64, early, pltpu.roll(late, 64, 1)).astype(BF)
            ft_ref[pair, 2 * v + 1] = jnp.where(lane < 64, pltpu.roll(early, 64, 1), late).astype(BF)
        target = ot_ref.at[
            pl.ds(pl.multiple_of(lax.rem(y, 2) * 448, 448), 448),
            pl.ds(pl.multiple_of((pair * 2 + c) * 128, 128), 128),
        ]
        own_core = y // 2
        for d in range(1, 4):
            to = around(y, d)
            send(
                ft_ref.at[pair, to], target, f_s.at[pair, d], f_r.at[pair, lax.rem(y, 2), c],
                y=to, c=own_core,
            )
        here = own_core == c

        @pl.when(here)
        def _():
            target[...] = ft_ref[pair, y]

        across = copy_to(
            ft_ref.at[pair, y], target, f_s.at[pair, 0], f_r.at[pair, lax.rem(y, 2), c], c=1 - c
        )

        @pl.when(jnp.logical_not(here))
        def _():
            across.start()

        returns.append((here, across))

    plan = {
        1: [(heads_done, 0)],
        2: [(partner_half, 0)],
        3: [(heads_done, 1), (pass_on, 0), (out_first,)],
        4: [(partner_half, 1)],
        5: [(heads_done, 2), (pass_on, 1), (out_second,)],
        6: [(partner_half, 2)],
        7: [(heads_done, 3), (pass_on, 2), (out_ready,), (multiply, 0)],
        8: [(partner_half, 3), (add_far, 0), (multiply, 1)],
        9: [(pass_on, 3), (add_near, 0), (add_far, 1), (multiply, 2)],
        10: [(multiply, 3), (add_near, 1), (add_far, 2)],
        11: [(add_near, 2), (add_far, 3)],
        12: [(add_near, 3)],
    }
    for slot in range(13):
        if slot < 8:
            lax.fori_loop(slot * 2, slot * 2 + 2, two, 0)
        for event, *which in plan.get(slot, []):
            event(*which)

    for pair in range(2):
        for ys in range(2):
            for cs in range(2):
                mine = (c * 2 + ys == y) & (c == cs)

                @pl.when(jnp.logical_not(mine))
                def _():
                    block = ot_ref.at[
                        ys * 448 : ys * 448 + 448, (pair * 2 + cs) * 128 : (pair * 2 + cs) * 128 + 128
                    ]
                    arrived(block, f_s.at[pair, 0], f_r.at[pair, ys, cs])

    def last(i, carry):
        rows = pl.ds(pl.multiple_of(i * 128, 128), 128)
        out_ref[rows, :] = nt(sel_ref[rows, :], ot_ref[...]).astype(BF)
        return carry

    lax.fori_loop(0, 4, last, 0)
    for made in sends:
        made.wait_send()
    for here, across in returns:

        @pl.when(jnp.logical_not(here))
        def _():
            across.wait_send()


def layer(uq, wk, wv, wo, q, latk, ropk, selk, sel, cos, sin, lengths, cache_latent, cache_rope):
    vmem = pl.BlockSpec(memory_space=pltpu.VMEM)
    hbm = pl.BlockSpec(memory_space=pl.ANY)
    dma = pltpu.SemaphoreType.DMA
    scratch = [
        ((8, 16, 1792), F32), ((8, 16, 1792), BF), ((8, 16, 1792), BF),
        ((8, 56, 1024), BF), ((8, 56, 1024), BF),
        ((4, 4, 128, 1664), BF), ((2, 4, 448, 1024), BF),
        ((3, 8, 128), F32), ((8, 8, 128), F32), ((4, 8, 128), F32), ((4, 8, 128), F32),
        ((TOK, QRANK), BF), ((TOK, KVRANK), BF), ((TOK, 256), BF),
        ((HL, TOK, KVRANK), BF), ((HL, TOK, 256), BF), ((HL, TOK, KVRANK), BF),
        ((SLOTS, 4, CACHE, KVRANK), BF), ((SLOTS, 4, ROPE, CACHE), BF),
        ((128, CACHE), F32), ((128, 16), F32), ((128, CACHE), F32), ((128, 16), F32),
        ((4, 2, HALF, 1024), BF), ((4, 4, 2, HALF, 1024), BF),
        ((4, 4, 448, 256), BF), ((4, 2, 224, 256), BF), ((4, 2, 448, 256), BF),
        ((2, 448, 256), F32), ((2, 4, 448, 128), BF), ((896, TOK), BF),
    ]
    counts = [
        (SLOTS,), (SLOTS,), (8,), (8,), (8,), (8,), (8,), (8,), (2, 4), (2, 4), (40,), (40,),
        (4,), (4,), (4,), (4,), (4,), (4,), (4, 6), (4, 6), (4, 2), (4, 2), (4, 2), (4, 2),
        (2, 4), (2, 2, 2),
    ]
    return pl.pallas_call(
        layer_kernel,
        out_shape=(jax.ShapeDtypeStruct((TOK, 896), BF), jax.ShapeDtypeStruct((8, 128), F32)),
        in_specs=[vmem] * 11 + [pl.BlockSpec(memory_space=pltpu.SMEM), hbm, hbm],
        out_specs=(vmem, vmem),
        scratch_shapes=[pltpu.VMEM(s, d) for s, d in scratch] + [dma(n) for n in counts],
        compiler_params=pltpu.CompilerParams(
            vmem_limit_bytes=67043328, collective_id=0, has_side_effects=True
        ),
        name="layer",
    )(uq, wk, wv, wo, q, latk, ropk, selk, sel, cos, sin, lengths, cache_latent, cache_rope)


def tables(lengths):
    half = ROPE // 2
    frequency = 10000.0 ** (-jnp.arange(half, dtype=F32) / half)
    frequency = jnp.tile(frequency, 4)
    positions = (lengths[:, None] + jnp.arange(NEWTOK, dtype=jnp.int32)[None, :]).reshape(TOK, 1)
    angles = positions.astype(F32) * frequency[None, :]
    sign = jnp.where(jnp.arange(128) % 64 < 32, -1.0, 1.0).astype(F32)
    return jnp.cos(angles), jnp.sin(angles) * sign[None, :]


def shards(q_latent, new_latent, new_rope, cache_latent, cache_rope, lengths, assignment, w_uq, w_uk, w_uv, w_o):
    slot_of = assignment[0]
    at = jnp.arange(TOK, dtype=jnp.int32)
    selk = (
        (jnp.tile(slot_of, NEWTOK)[None, :] == at[:, None] // 4)
        & (at[None, :] // SEQS == at[:, None] % 4)
    ).astype(BF)
    held = (at // 256) * 256 + ((at // 64) % 2) * 128 + ((at // 128) % 2) * 64 + at % 64
    sel = (
        (jnp.repeat(slot_of, NEWTOK)[:, None] == held[None, :] // 4)
        & (at[:, None] % 4 == held[None, :] % 4)
    ).astype(BF)
    cos, sin = tables(lengths)
    out, norm = layer(
        w_uq, w_uk, w_uv, w_o.T,
        q_latent.transpose(1, 0, 2).reshape(TOK, QRANK),
        new_latent.transpose(1, 0, 2).reshape(TOK, KVRANK),
        new_rope.transpose(1, 2, 0), selk, sel, cos, sin, lengths, cache_latent, cache_rope,
    )
    return out.reshape(SEQS, NEWTOK, 896), norm[0, 0:1]


def solution(mesh):
    split = Mesh(mesh.devices.reshape(4, 4, 4, 2), ("dp_0", "dp_1", "tp_0", "tp_1"))
    dp, tp = ("dp_0", "dp_1"), ("tp_0", "tp_1")
    placed = (
        P(dp, None, None), P(dp, None, None), P(dp, None, None), P(dp, None, None), P(dp, None, None),
        P(dp), P(dp, None), P(dp + tp, None), P(dp + tp, None), P(dp + tp, None), P(None, dp + tp),
    )
    return jax.shard_map(
        shards, mesh=split, in_specs=placed, out_specs=(P(dp, None, tp), P()), check_vma=False
    )
```

```python
import jax
import jax.numpy as jnp
import numpy as np
from jax import lax
from jax.experimental import pallas as pl
from jax.experimental.pallas import tpu as pltpu
from jax.sharding import Mesh
from jax.sharding import PartitionSpec as P

D = 7168
QRANK = 1536
KVRANK = 512
NOPE = 128
ROPE = 64
VDIM = 128
HEADS = 64
NEWTOK = 4
CACHE = 256
SEQS = 128
TOK = SEQS * NEWTOK
HL = 8
GROUPS = SEQS // 4
SLOTS = 4
BF = jnp.bfloat16
F32 = jnp.float32
DP_TP = ("dp_0", "dp_1", "tp_0", "tp_1")
TP = ("tp_0", "tp_1")
DP = ("dp_0", "dp_1")
SCALE = (NOPE + ROPE) ** (-0.5)


def nt(a, b):
    return lax.dot_general(a, b, (((1,), (1,)), ((), ())), preferred_element_type=F32)


def nn(a, b):
    return lax.dot_general(a, b, (((1,), (0,)), ((), ())), preferred_element_type=F32)


def project(q_ref, u_ref, cos_ref, sin_ref, abs_ref, qr_ref, part):
    def nope_pair(i):
        cols = pl.ds(i * 256, 256)
        both = nn(q_ref[...], u_ref[:, 0:96, cols].reshape(QRANK, 256)).astype(BF)
        for j in range(2):
            own_cols = pl.ds(i * 256 + j * 128, 128)
            keys = u_ref[:, 96:128, own_cols].reshape(KVRANK, 128)
            abs_ref[i * 2 + j] = nt(both[:, j * 128 : (j + 1) * 128], keys).astype(BF)

    lane = lax.broadcasted_iota(jnp.int32, (TOK, 128), 1)
    row = lax.broadcasted_iota(jnp.int32, (TOK, 128), 0)
    own = lax.rem(row // 4, 4)
    low = lax.rem(lane, 64) < 32

    def quad(i):
        nope_pair(2 * i)
        nope_pair(2 * i + 1)
        if i == 0:
            pe_cols = u_ref[:, 0:96, 1024:1280].reshape(QRANK, 256)
        else:
            tail = [u_ref[:, 96:128, 1024 + b * 128 : 1152 + b * 128] for b in range(3)]
            pe_cols = jnp.concatenate(
                [
                    u_ref[:, 0:96, 1280:1408].reshape(QRANK, 128),
                    jnp.concatenate(tail, axis=1).reshape(QRANK, 128),
                ],
                axis=1,
            )
        four = nn(q_ref[...], pe_cols).astype(BF).astype(F32)
        for j in range(2):
            pe = four[:, j * 128 : (j + 1) * 128]
            other = jnp.where(low, pltpu.roll(pe, 96, 1), pltpu.roll(pe, 32, 1))
            rot = pe * cos_ref[...] + other * sin_ref[...]
            flip = pltpu.roll(rot, 64, 1)
            for odd in range(2):
                twice = jnp.where((lane < 64) == (odd == 0), rot, flip)
                head = i * 4 + j * 2 + odd
                for half in range(2):
                    kept = jnp.where(own == 2 * half + lane // 64, twice, 0.0)
                    qr_ref[head, :, half * 128 : (half + 1) * 128] = kept.astype(BF)

    quad(part)


def scores_of(g, abs_ref, qr_ref, latn_ref, ropn_ref, lat, rop, sc_ref, scn_ref):
    rows = pl.ds(pl.multiple_of(g * 16, 16), 16)
    q = abs_ref[:, rows, :].reshape(128, KVRANK)
    qr = qr_ref[:, rows, :].reshape(128, 256)
    seq = lax.rem(lax.broadcasted_iota(jnp.int32, (128, KVRANK), 0) // 4, 4)
    zero = jnp.zeros_like(q)
    parts = jnp.concatenate([jnp.where(seq == s, q, zero) for s in range(4)], axis=1)
    keys = jnp.concatenate([lat[s] for s in range(4)], axis=1)
    sc_ref[...] = nt(parts, keys) + nn(qr, rop[...].reshape(256, CACHE))
    scn_ref[...] = nt(q, latn_ref[rows, :]) + nt(qr, ropn_ref[rows, :])


def attend(g, len_ref, latn_ref, lat, sc_ref, scn_ref, lo_ref):
    row = lax.broadcasted_iota(jnp.int32, (128, CACHE), 0)
    seq = lax.rem(row // 4, 4)
    limit = jnp.where(
        seq == 0,
        len_ref[g * 4],
        jnp.where(
            seq == 1, len_ref[g * 4 + 1], jnp.where(seq == 2, len_ref[g * 4 + 2], len_ref[g * 4 + 3])
        ),
    )
    at = lax.broadcasted_iota(jnp.int32, (128, CACHE), 1)
    sc = jnp.where(at < limit, sc_ref[...] * SCALE, -jnp.inf)
    nrow = lax.broadcasted_iota(jnp.int32, (128, 16), 0)
    ncol = lax.broadcasted_iota(jnp.int32, (128, 16), 1)
    fits = (lax.rem(nrow // 4, 4) == ncol // 4) & (lax.rem(ncol, 4) <= lax.rem(nrow, 4))
    scn = jnp.where(fits, scn_ref[...] * SCALE, -jnp.inf)
    top = jnp.maximum(
        jnp.max(sc, axis=1, keepdims=True), jnp.max(scn, axis=1, keepdims=True)
    )
    ex = jnp.exp(sc - top)
    exn = jnp.exp(scn - top)
    total = jnp.sum(ex, axis=1, keepdims=True) + jnp.sum(exn, axis=1, keepdims=True)
    share = 1.0 / total
    w = (ex * share).astype(BF)
    wn = (exn * share).astype(BF)
    zero = jnp.zeros_like(w)
    parts = jnp.concatenate([jnp.where(seq == s, w, zero) for s in range(4)], axis=1)
    rows = pl.ds(pl.multiple_of(g * 16, 16), 16)
    out = nn(parts, lat[...].reshape(4 * CACHE, KVRANK)) + nn(wn, latn_ref[rows, :])
    lo_ref[:, rows, :] = out.astype(BF).reshape(HL, 16, KVRANK)


MESH = pl.DeviceIdType.MESH
CHUNKS = 4
HALF = 64


def around(i, d):
    return lax.rem(i + d + 4, 4)


def layer_kernel(
    ropk_ref, asn_ref, lenv_ref, freq_ref, len_ref,
    uq_hbm, wk_hbm, wv_hbm, wo_hbm, q_hbm, latk_hbm, lat_hbm, rop_hbm,
    out_hbm, sel_hbm, norm_ref,
    uq_ref, wk_ref, wv_ref, wo_ref, q_ref, latk_ref, selk_ref, sel_ref, cos_ref, sin_ref,
    stage, packs, rp, opack, orp, u_ref, v_ref, wo_all, nsend, ntp, ny, nz,
    qs_ref, latn_ref, ropn_ref, abs_ref, qr_ref, lo_ref, lat_ref, rop_ref, sc0, scn0, sc1, scn1,
    ho_ref, hb_ref, ct_ref, r1_ref, rx_ref, fs_ref, ft_ref, ot_ref,
    in_sem, lat_sem, rop_sem, a2a_sem, o2a_sem, nt_sem, nyz_sem, ag_s, ag_r, uv_s, uv_r,
    oz_sem, od_sem, d2_s, d2_r, hy_s, hy_r, r1_s, r1_r, r2_s, r2_r, f_sem,
):
    z, y = lax.axis_index("dp_0"), lax.axis_index("dp_1")
    x, c = lax.axis_index("tp_0"), lax.axis_index("tp_1")
    t = x * 2 + c
    def copy_to(src, dst, ss, rs, **axes):
        names = {"z": "dp_0", "y": "dp_1", "x": "tp_0", "c": "tp_1"}
        return pltpu.make_async_remote_copy(
            src_ref=src, dst_ref=dst, send_sem=ss, recv_sem=rs,
            device_id={names[n]: v for n, v in axes.items()}, device_id_type=MESH,
        )

    def send(src, dst, ss, rs, **axes):
        copy_to(src, dst, ss, rs, **axes).start()

    def arrived(dst, rs):
        copy_to(dst, dst, rs, rs, c=1 - c).wait_recv()

    def left(src, ss):
        copy_to(src, src, ss, ss, c=1 - c).wait_send()

    barrier = pltpu.get_barrier_semaphore()

    def greet(**axes):
        names = {"z": "dp_0", "y": "dp_1", "x": "tp_0", "c": "tp_1"}
        pl.semaphore_signal(
            barrier, inc=1, device_id={names[n]: v for n, v in axes.items()}, device_id_type=MESH
        )

    for dt in range(1, 8):
        peer = lax.rem(t + dt, 8)
        greet(x=peer // 2, c=lax.rem(peer, 2))
    for d in range(1, 4):
        greet(z=around(z, d))
        greet(y=around(y, d))
        greet(y=around(y, d), c=1 - c)

    loads = []
    for n, (src, dst) in enumerate(
        (
            (uq_hbm, uq_ref), (wk_hbm, wk_ref), (wv_hbm, wv_ref), (wo_hbm, wo_ref), (q_hbm, q_ref),
            (latk_hbm, latk_ref),
        )
    ):
        loads.append(pltpu.make_async_copy(src, dst, in_sem.at[n]))
        loads[n].start()

    def fetch(g):
        slot = lax.rem(g, SLOTS)
        return (
            pltpu.make_async_copy(lat_hbm.at[pl.ds(g * 4, 4)], lat_ref.at[slot], lat_sem.at[slot]),
            pltpu.make_async_copy(rop_hbm.at[pl.ds(g * 4, 4)], rop_ref.at[slot], rop_sem.at[slot]),
        )

    def start(g):
        for made in fetch(g):
            made.start()

    def wait(g):
        for made in fetch(g):
            made.wait()

    for g in range(SLOTS - 1):
        start(g)

    lane12 = lax.broadcasted_iota(jnp.int32, (12, 128), 1)

    def fold(v):
        rows, cols = v.shape
        total = jnp.zeros((8, 128), F32)
        for i in range(rows // 8):
            for j in range(cols // 128):
                part = v[i * 8 : i * 8 + 8, j * 128 : j * 128 + 128]
                total = total + part * part
        return total

    def pack_one(p, squares):
        for i in range(4):
            v = uq_ref[:, pl.ds(pl.multiple_of(p * 1536 + i * 384, 128), 384)]
            v0, v1, v2 = v[:, 0:128], v[:, 128:256], v[:, 256:384]
            stage[p, 0:12, i * 256 : i * 256 + 128] = v0
            stage[p, 0:12, i * 256 + 128 : i * 256 + 256] = pltpu.roll(
                jnp.where(lane12 < 64, v2, v1), 64, 1
            )
            stage[p, 0:12, 1024 + i * 128 : 1152 + i * 128] = jnp.where(lane12 < 64, v1, v2)
            stage[p, i * 4 : i * 4 + 4, 1536:1792] = wv_ref[
                :, pl.ds(pl.multiple_of(p * 1024 + i * 256, 128), 256)
            ]
        stage[p, 12:16, 0:1024] = wk_ref[:, pl.ds(pl.multiple_of(p * 1024, 128), 1024)]
        stage[p, 12:16, 1024:1536] = jnp.zeros((4, 512), F32)
        whole = stage[p]
        packs[p] = whole.astype(BF)
        return squares + fold(whole)

    for n in range(3):
        loads[n].wait()
    squares = lax.fori_loop(0, 8, pack_one, jnp.zeros((8, 128), F32))
    pl.semaphore_wait(barrier, 16)
    for dt in range(1, 8):
        peer = lax.rem(t + dt, 8)
        send(
            packs.at[peer], rp.at[t], a2a_sem.at[0], a2a_sem.at[1], x=peer // 2, c=lax.rem(peer, 2)
        )
    rp[t] = packs[t]

    def pack_out(p, squares):
        v = wo_ref[:, pl.ds(pl.multiple_of(p * 1024, 128), 1024)]
        opack[p] = v.astype(BF)
        return squares + fold(v)

    loads[3].wait()
    squares = lax.fori_loop(0, 8, pack_out, squares)
    nsend[0] = squares
    ntp[t] = squares
    for dt in range(1, 8):
        peer = lax.rem(t + dt, 8)
        where = dict(x=peer // 2, c=lax.rem(peer, 2))
        send(nsend.at[0], ntp.at[t], nt_sem.at[0], nt_sem.at[1], **where)
        send(opack.at[peer], orp.at[t], o2a_sem.at[0], o2a_sem.at[1], **where)
    orp[t] = opack[t]

    row = lax.broadcasted_iota(jnp.int32, (TOK, TOK), 0)
    col = lax.broadcasted_iota(jnp.int32, (TOK, TOK), 1)
    spread = jnp.where(
        lax.broadcasted_iota(jnp.int32, (SEQS, TOK), 0)
        == lax.broadcasted_iota(jnp.int32, (SEQS, TOK), 1) // NEWTOK, 1.0, 0.0,
    ).astype(BF)
    slot_of = jnp.broadcast_to(asn_ref[...], (8, SEQS)).astype(F32)
    slot_by_token = nn(slot_of.astype(BF), spread)[0:1, :].astype(jnp.int32)
    slot_tiled = jnp.concatenate([asn_ref[...]] * NEWTOK, axis=1)
    selk_ref[0] = jnp.where(
        (slot_tiled == row // 4) & (col // SEQS == lax.rem(row, 4)), 1.0, 0.0
    ).astype(BF)
    same_token = lax.rem(row, 4) == lax.rem(col, 4)
    selk_ref[1] = jnp.where((slot_by_token == row // 4) & same_token, 1.0, 0.0).astype(BF)
    held = (
        (row // 256) * 256 + lax.rem(row // 64, 2) * 128 + lax.rem(row // 128, 2) * 64
        + lax.rem(row, 64)
    )
    back = jnp.where((slot_by_token == held // 4) & same_token, 1.0, 0.0).astype(BF)
    identity = jnp.where(row == col, 1.0, 0.0).astype(BF)
    sel_ref[...] = nt(identity, back).astype(BF)
    keep_sel = pltpu.make_async_copy(sel_ref, sel_hbm, in_sem.at[6])
    keep_out = pltpu.make_async_copy(ot_ref, out_hbm, in_sem.at[7])
    lengths_wide = jnp.broadcast_to(lenv_ref[...], (SEQS, SEQS)).astype(F32).astype(BF)

    def rotation(i, carry):
        rows = pl.ds(pl.multiple_of(i * 128, 128), 128)
        r = lax.broadcasted_iota(jnp.int32, (128, 128), 0) + i * 128
        lane = lax.broadcasted_iota(jnp.int32, (128, 128), 1)
        pick = jnp.where(r // 4 == lane, 1.0, 0.0).astype(BF)
        positions = nt(pick, lengths_wide) + lax.rem(r, 4).astype(F32)
        angles = positions * freq_ref[0:1, :]
        cos_ref[rows, :] = jnp.cos(angles)
        sine = jnp.sin(angles)
        sin_ref[rows, :] = jnp.where(lax.rem(lane, 64) < 32, -sine, sine)
        return carry

    arrived(rp.at[0:7], a2a_sem.at[1])
    big = rp[...].reshape(128, 1792)
    r = lax.broadcasted_iota(jnp.int32, (128, 128), 0)
    col = lax.broadcasted_iota(jnp.int32, (128, 128), 1)
    origin = jnp.where(
        r < 96, (r // 12) * 16 + lax.rem(r, 12), ((r - 96) // 4) * 16 + 12 + lax.rem(r - 96, 4)
    )
    order = jnp.where(col == origin, 1.0, 0.0).astype(BF)
    sorted_rows = nn(order, big[:, 0:1536]).astype(BF)
    r32 = lax.broadcasted_iota(jnp.int32, (32, 128), 0)
    col32 = lax.broadcasted_iota(jnp.int32, (32, 128), 1)
    uv_parts = []
    for i in range(4):
        pick = jnp.where(col32 == (r32 // 4) * 16 + i * 4 + lax.rem(r32, 4), 1.0, 0.0).astype(BF)
        uv_parts.append(nn(pick, big[:, 1536:1792]).astype(BF))
    me = z * 4 + y
    u_ref[me, 0:96] = sorted_rows[0:96, 0:1408]
    u_ref[me, 96:128, 0:1024] = sorted_rows[96:128, 0:1024]
    for i in range(3):
        u_ref[me, 96:128, 1024 + i * 128 : 1152 + i * 128] = sorted_rows[
            i * 32 : i * 32 + 32, 1408:1536
        ]
    v_ref[me] = jnp.concatenate(uv_parts, axis=1)

    def piece(ring, ia, ib, sub=None):
        if ring == 2:
            at = v_ref.at[ia * 4 + ib]
            return at if sub is None else at.at[:, pl.ds(sub * 512, 512)]
        rows = pl.ds(ring * 64, 64) if sub is None else pl.ds(ring * 64 + sub * 32, 32)
        return u_ref.at[ib * 4 + ia if ring == 0 else ia * 4 + ib, rows]

    def step(ring, along_first, to):
        first, second = ("y", "z") if ring == 0 else ("z", "y")
        return {first if along_first else second: to}

    where_a = [y, z, z]
    where_b = [z, y, y]

    def sent(ring):
        return ag_s.at[0] if ring < 2 else uv_s.at[0]

    def got(ring, n):
        if ring == 2:
            return uv_r.at[min(n, 12)]
        return ag_r.at[24 if n >= 12 else ring * 12 + n]

    offsets = (0, -1, 1, 2)

    def first_send(ring):
        a, b = where_a[ring], where_b[ring]
        for k, d in enumerate((1, -1)):
            ref = piece(ring, a, b)
            send(ref, ref, sent(ring), got(ring, k), **step(ring, True, around(a, d)))

    def first_forward(ring):
        a, b = where_a[ring], where_b[ring]
        for k, d in enumerate((1, -1)):
            arrived(piece(ring, around(a, -d), b), got(ring, k))
            ref = piece(ring, around(a, -d), b, k)
            send(ref, ref, sent(ring), got(ring, 2 + k), **step(ring, True, around(a, d)))

    def first_last(ring):
        a, b = where_a[ring], where_b[ring]
        for k in range(2):
            arrived(piece(ring, around(a, 2), b, k), got(ring, 2 + k))

    def second_send(ring, p):
        a, b = where_a[ring], where_b[ring]
        ia = around(a, offsets[p])
        for k, d in enumerate((1, -1)):
            ref = piece(ring, ia, b)
            send(ref, ref, sent(ring), got(ring, 4 + p * 2 + k), **step(ring, False, around(b, d)))

    def second_forward(ring, p):
        a, b = where_a[ring], where_b[ring]
        ia = around(a, offsets[p])
        for k, d in enumerate((1, -1)):
            arrived(piece(ring, ia, around(b, -d)), got(ring, 4 + p * 2 + k))
            ref = piece(ring, ia, around(b, -d), k)
            send(ref, ref, sent(ring), got(ring, 12), **step(ring, False, around(b, d)))

    for ring in range(2):
        first_send(ring)
    for ring in range(2):
        second_send(ring, 0)

    loads[4].wait()
    loads[5].wait()
    keep_sel.start()

    def move_q(i, carry):
        cols = pl.ds(pl.multiple_of(i * 256, 256), 256)
        qs_ref[:, cols] = nn(selk_ref[1], q_ref[:, :, cols].reshape(TOK, 256)).astype(BF)
        return carry

    lax.fori_loop(0, QRANK // 256, move_q, 0)
    lax.fori_loop(0, 4, rotation, 0)

    arrived(ntp.at[0:7], nt_sem.at[1])
    line = ntp[0]
    for i in range(1, 8):
        line = line + ntp[i]
    latn_ref[...] = nn(selk_ref[1], latk_ref[...].reshape(TOK, KVRANK)).astype(BF)
    rope_rows = jnp.concatenate([ropk_ref[k] for k in range(4)], axis=1)
    ropn_ref[...] = nt(selk_ref[0], jnp.concatenate([rope_rows] * 4, axis=0)).astype(BF)
    nsend[1] = line
    ny[y] = line
    for d in range(1, 4):
        send(nsend.at[1], ny.at[y], nyz_sem.at[0], nyz_sem.at[1], y=around(y, d))

    for ring in range(2):
        first_forward(ring)
    for ring in range(2):
        second_send(ring, 1)
        second_send(ring, 2)
    first_send(2)
    for ring in range(2):
        second_forward(ring, 0)
    arrived(ny.at[0:3], nyz_sem.at[1])
    plane = ((ny[0] + ny[1]) + ny[2]) + ny[3]
    nsend[2] = plane
    nz[z] = plane
    for d in range(1, 4):
        send(nsend.at[2], nz.at[z], nyz_sem.at[0], nyz_sem.at[2], z=around(z, d))
    for ring in range(2):
        first_last(ring)
        second_send(ring, 3)
    first_forward(2)
    for p in range(1, 3):
        for ring in range(2):
            second_forward(ring, p)

    arrived(orp.at[0:7], o2a_sem.at[1])
    wo_all[c, z] = jnp.concatenate([orp[i].astype(F32) for i in range(8)], axis=0).astype(BF)
    first_last(2)
    for ring in range(2):
        second_forward(ring, 3)
    for p in range(4):
        second_send(2, p)
    send(wo_all.at[c, z], wo_all.at[c, z], od_sem.at[0], od_sem.at[1], c=1 - c)
    for later in range(2):
        for k, d in enumerate((1, -1)):
            part = wo_all.at[c, z, pl.ds((k ^ later) * 224, 224)]
            send(part, part, oz_sem.at[0], oz_sem.at[1 + later], z=around(z, d))
    arrived(u_ref.at[0:4], ag_r.at[24])
    arrived(nz.at[0:3], nyz_sem.at[2])
    everything = ((nz[0] + nz[1]) + nz[2]) + nz[3]
    everything = jnp.sum(jnp.sum(everything, axis=1, keepdims=True), axis=0, keepdims=True)
    entries = HEADS * (NOPE + ROPE) + 2 * HEADS * NOPE + D
    norm_ref[0] = jnp.sqrt(everything / entries)[0, 0]

    project(qs_ref, u_ref, cos_ref, sin_ref, abs_ref, qr_ref, 0)
    second_forward(2, 0)
    second_forward(2, 1)
    project(qs_ref, u_ref, cos_ref, sin_ref, abs_ref, qr_ref, 1)
    second_forward(2, 2)

    def score(g, sc, scn):
        slot = lax.rem(g, SLOTS)
        scores_of(g, abs_ref, qr_ref, latn_ref, ropn_ref, lat_ref.at[slot], rop_ref.at[slot], sc, scn)

    def finish(g, sc, scn):
        attend(g, len_ref, latn_ref, lat_ref.at[lax.rem(g, SLOTS)], sc, scn, lo_ref)

    wait(0)
    score(0, sc0, scn0)

    def two(i):
        g = i * 2

        @pl.when(g + 3 < GROUPS)
        def _():
            start(g + 3)

        wait(g + 1)
        score(g + 1, sc1, scn1)
        finish(g, sc0, scn0)

        @pl.when(g + 4 < GROUPS)
        def _():
            start(g + 4)

        @pl.when(g + 2 < GROUPS)
        def _():
            wait(g + 2)

        score(jnp.minimum(g + 2, GROUPS - 1), sc0, scn0)
        finish(g + 1, sc1, scn1)

    def values_pass():
        second_forward(2, 3)

    def values_ready():
        arrived(v_ref.at[0:4], uv_r.at[12])

    def out_pass():
        arrived(wo_all.at[c, z], oz_sem.at[1])
        for k, d in enumerate((1, -1)):
            part = wo_all.at[c, around(z, -d), pl.ds(k * 224, 224)]
            send(part, part, oz_sem.at[0], oz_sem.at[3], z=around(z, d))

    def out_near():
        arrived(wo_all.at[c, z], oz_sem.at[2])
        for d in (1, -1):
            near = wo_all.at[c, around(z, d)]
            send(near, near, od_sem.at[0], od_sem.at[1], c=1 - c)

    def out_far():
        far = wo_all.at[c, around(z, 2)]
        arrived(far, oz_sem.at[3])
        send(far, far, od_sem.at[0], od_sem.at[1], c=1 - c)

    def out_ready():
        arrived(wo_all.at[1 - c], od_sem.at[1])

    def head_values(j):
        rows = slice(j * 128, j * 128 + 128)
        for h in range(HL):
            up = v_ref[:, :, h * 128 : h * 128 + 128].reshape(KVRANK, 128)
            both = nn(lo_ref[h, rows, :], up).astype(BF)
            for half in range(2):
                ho_ref[j, half, :, h * 128 : h * 128 + 128] = both[half * 64 : half * 64 + 64]
        hb_ref[j, y, c] = ho_ref[j, c]

    def heads_done(j):
        head_values(j)
        send(ho_ref.at[j, 1 - c], hb_ref.at[j, y, c], d2_s.at[0], d2_r.at[j], c=1 - c)
        for d in (1, -1):
            send(ho_ref.at[j, c], hb_ref.at[j, y, c], hy_s.at[0], hy_r.at[j, 0], y=around(y, d))

    def partner_half(j):
        ref = hb_ref.at[j, y, 1 - c]
        arrived(ref, d2_r.at[j])
        for d in (1, -1):
            send(ref, ref, hy_s.at[0], hy_r.at[j, 0], y=around(y, d))

    def pass_on(j):
        arrived(hb_ref.at[j, 0:2], hy_r.at[j, 0])
        for k, d in enumerate((1, -1)):
            ref = hb_ref.at[j, around(y, -d), k]
            send(ref, ref, hy_s.at[0], hy_r.at[j, 1], y=around(y, d))

    def multiply(j):
        arrived(hb_ref.at[j, around(y, 2)], hy_r.at[j, 1])

        def block(n):
            zs = lax.rem(x + n, 4)
            tokens = jnp.concatenate(
                [hb_ref[j, :, k].reshape(4 * HALF, 1024) for k in range(2)], axis=1
            )
            columns = jnp.concatenate([wo_all[k, zs] for k in range(2)], axis=1)
            ct_ref[j, zs] = nt(columns, tokens).astype(BF)

        block(2)
        for k, d in enumerate((1, -1)):
            send(
                ct_ref.at[j, around(x, 2), pl.ds(k * 224, 224)], r1_ref.at[j, k],
                r1_s.at[0], r1_r.at[j], x=around(x, d),
            )

        def rest(n, carry):
            block(jnp.where(n == 0, 1, jnp.where(n == 1, 3, 0)))
            return carry

        lax.fori_loop(0, 3, rest, 0)

    def add_far(j):
        arrived(r1_ref.at[j], r1_r.at[j])
        for k, d in enumerate((1, -1)):
            rows = slice(k * 224, k * 224 + 224)
            near = around(x, d)
            both = ct_ref[j, near, rows].astype(F32) + r1_ref[j, k].astype(F32)
            ct_ref[j, near, rows] = both.astype(BF)
            send(ct_ref.at[j, near], rx_ref.at[j, k], r2_s.at[0], r2_r.at[j], x=near)

    def collect(j):
        fs_ref[j % 2] = (
            ct_ref[j, x].astype(F32) + rx_ref[j, 0].astype(F32) + rx_ref[j, 1].astype(F32)
        )
        if j % 2 == 0:
            return
        lane = lax.broadcasted_iota(jnp.int32, (448, 128), 1)
        for v in range(2):
            early = fs_ref[0, :, v * 128 : v * 128 + 128]
            late = fs_ref[1, :, v * 128 : v * 128 + 128]
            ft_ref[j // 2 * 4 + 2 * v] = jnp.where(lane < 64, early, pltpu.roll(late, 64, 1)).astype(BF)
            ft_ref[j // 2 * 4 + 2 * v + 1] = jnp.where(lane < 64, pltpu.roll(early, 64, 1), late).astype(BF)

    here = y // 2 == c

    def add_near(j):
        arrived(rx_ref.at[j], r2_r.at[j])
        collect(j)
        if j % 2 == 0:
            return
        pair = j // 2
        target = ot_ref.at[
            pl.ds(pl.multiple_of(lax.rem(y, 2) * 448, 448), 448),
            pl.ds(pl.multiple_of((pair * 2 + c) * 128, 128), 128),
        ]
        for d in (2, 1, 3):
            to = around(y, d)
            send(ft_ref.at[pair * 4 + to], target, f_sem.at[0], f_sem.at[1], y=to, c=y // 2)

        @pl.when(here)
        def _():
            target[...] = ft_ref[pair * 4 + y]

        @pl.when(jnp.logical_not(here))
        def _():
            send(ft_ref.at[pair * 4 + y], target, f_sem.at[2], f_sem.at[1], c=1 - c)

    plan = {
        0: [(values_pass,), (out_pass,)],
        3: [(values_ready,), (heads_done, 0)],
        4: [(partner_half, 0)],
        6: [(out_near,)],
        7: [(pass_on, 0), (heads_done, 1)],
        8: [(partner_half, 1)],
        11: [(heads_done, 2), (out_far,)],
        12: [(pass_on, 1), (partner_half, 2), (out_ready,), (multiply, 0)],
        13: [(add_far, 0)],
        14: [(multiply, 1)],
        15: [(pass_on, 2), (heads_done, 3)],
        16: [(add_near, 0), (partner_half, 3), (add_far, 1)],
        17: [(multiply, 2)],
        18: [(pass_on, 3), (add_near, 1), (add_far, 2)],
        19: [(multiply, 3)],
        20: [(add_near, 2), (add_far, 3), (add_near, 3)],
    }

    def run(events):
        for event, *which in events:
            event(*which)

    def together(i, carry):
        two(i)
        for slot in range(16):
            if slot in plan:

                @pl.when(i == slot)
                def _():
                    run(plan[slot])

        return carry

    lax.fori_loop(0, 16, together, 0)
    for slot in range(16, 21):
        run(plan[slot])

    @pl.when(here)
    def _():
        arrived(ft_ref.at[0:6], f_sem.at[1])

    @pl.when(jnp.logical_not(here))
    def _():
        arrived(ft_ref.at[0:8], f_sem.at[1])

    keep_out.start()
    left(packs.at[0:7], a2a_sem.at[0])
    left(opack.at[0:7], o2a_sem.at[0])
    left(ntp.at[0:7], nt_sem.at[0])
    left(ntp.at[0:6], nyz_sem.at[0])
    left(u_ref.at[0:15], ag_s.at[0])
    left(v_ref.at[0:15], uv_s.at[0])
    left(wo_all.at[0, 0:3], oz_sem.at[0])
    left(wo_all.at[0], od_sem.at[0])
    left(ho_ref.at[0:2], d2_s.at[0])
    left(hb_ref.at[0:3], hy_s.at[0])
    left(ct_ref.at[0], r1_s.at[0])
    left(ct_ref.at[0:2], r2_s.at[0])
    left(ft_ref.at[0:6], f_sem.at[0])

    @pl.when(jnp.logical_not(here))
    def _():
        left(ft_ref.at[0:2], f_sem.at[2])

    keep_sel.wait()
    keep_out.wait()


def place_kernel(sel_ref, held_ref, out_ref):
    placed = nt(sel_ref[...], held_ref[...]).astype(BF)
    out_ref[...] = placed.reshape(32, 4, 896)


def layer(uq, wk, wv, wo, q, latk, ropk, slot_of, lengths, frequency, cache_latent, cache_rope):
    vmem = pl.BlockSpec(memory_space=pltpu.VMEM)
    smem = pl.BlockSpec(memory_space=pltpu.SMEM)
    hbm = pl.BlockSpec(memory_space=pl.ANY)
    dma = pltpu.SemaphoreType.DMA
    scratch = [
        ((12, 12288), F32), ((4, 8192), F32), ((4, 8192), F32), ((56, 8192), F32),
        ((SEQS, 4, QRANK), BF), ((SEQS, 4, KVRANK), BF), ((2, TOK, TOK), BF), ((TOK, TOK), BF),
        ((TOK, 128), F32), ((TOK, 128), F32),
        ((8, 16, 1792), F32), ((8, 16, 1792), BF), ((8, 16, 1792), BF),
        ((8, 56, 1024), BF), ((8, 56, 1024), BF),
        ((16, 128, 1408), BF), ((16, 32, 1024), BF), ((2, 4, 448, 1024), BF),
        ((3, 8, 128), F32), ((8, 8, 128), F32), ((4, 8, 128), F32), ((4, 8, 128), F32),
        ((TOK, QRANK), BF), ((TOK, KVRANK), BF), ((TOK, 256), BF),
        ((HL, TOK, KVRANK), BF), ((HL, TOK, 256), BF), ((HL, TOK, KVRANK), BF),
        ((SLOTS, 4, CACHE, KVRANK), BF), ((SLOTS, 4, ROPE, CACHE), BF),
        ((128, CACHE), F32), ((128, 16), F32), ((128, CACHE), F32), ((128, 16), F32),
        ((4, 2, HALF, 1024), BF), ((4, 4, 2, HALF, 1024), BF),
        ((4, 4, 448, 256), BF), ((4, 2, 224, 256), BF), ((4, 2, 448, 256), BF),
        ((2, 448, 256), F32), ((8, 448, 128), BF), ((896, TOK), BF),
    ]
    counts = [
        (8,), (SLOTS,), (SLOTS,), (2,), (2,), (2,), (3,), (1,), (25,), (1,), (13,),
        (4,), (2,), (1,), (4,), (1,), (4, 2), (1,), (4,), (1,), (4,), (3,),
    ]
    return pl.pallas_call(
        layer_kernel,
        out_shape=(
            jax.ShapeDtypeStruct((896, TOK), BF), jax.ShapeDtypeStruct((TOK, TOK), BF),
            jax.ShapeDtypeStruct((1,), F32),
        ),
        in_specs=[vmem] * 4 + [smem] + [hbm] * 8,
        out_specs=(hbm, hbm, smem),
        scratch_shapes=[pltpu.VMEM(s, d) for s, d in scratch] + [dma(n) for n in counts],
        compiler_params=pltpu.CompilerParams(
            vmem_limit_bytes=67043328, collective_id=0, has_side_effects=True
        ),
        name="layer",
    )(
        ropk, slot_of, lengths.reshape(1, SEQS), frequency, lengths,
        uq, wk, wv, wo, q, latk, cache_latent, cache_rope,
    )


def shards(q_latent, new_latent, new_rope, cache_latent, cache_rope, lengths, assignment, w_uq, w_uk, w_uv, w_o):
    half = ROPE // 2
    frequency = 10000.0 ** (-np.arange(half, dtype=np.float32) / half)
    frequency = np.broadcast_to(np.tile(frequency, 4)[None, :], (8, 128)).astype(np.float32)
    held, sel, norm = layer(
        w_uq, w_uk, w_uv, w_o.T, q_latent, new_latent, new_rope.transpose(1, 2, 0), assignment,
        lengths, jnp.asarray(frequency), cache_latent, cache_rope,
    )
    out = pl.pallas_call(
        place_kernel,
        out_shape=jax.ShapeDtypeStruct((SEQS, NEWTOK, 896), BF),
        grid=(4,),
        in_specs=[
            pl.BlockSpec((128, TOK), lambda i: (i, 0)), pl.BlockSpec((896, TOK), lambda i: (0, 0))
        ],
        out_specs=pl.BlockSpec((32, NEWTOK, 896), lambda i: (i, 0, 0)),
        name="place",
    )(sel, held)
    return out, norm


def solution(mesh):
    split = Mesh(mesh.devices.reshape(4, 4, 4, 2), ("dp_0", "dp_1", "tp_0", "tp_1"))
    dp, tp = ("dp_0", "dp_1"), ("tp_0", "tp_1")
    placed = (
        P(dp, None, None), P(dp, None, None), P(dp, None, None), P(dp, None, None), P(dp, None, None),
        P(dp), P(dp, None), P(dp + tp, None), P(dp + tp, None), P(dp + tp, None), P(None, dp + tp),
    )
    return jax.shard_map(
        shards, mesh=split, in_specs=placed, out_specs=(P(dp, None, tp), P()), check_vma=False
    )
```

```python
import jax
import jax.numpy as jnp
import numpy as np
from jax import lax
from jax.experimental import pallas as pl
from jax.experimental.pallas import tpu as pltpu
from jax.sharding import Mesh
from jax.sharding import PartitionSpec as P

D = 7168
QRANK = 1536
KVRANK = 512
NOPE = 128
ROPE = 64
VDIM = 128
HEADS = 64
NEWTOK = 4
CACHE = 256
SEQS = 128
TOK = SEQS * NEWTOK
HL = 8
GROUPS = SEQS // 4
SLOTS = 4
BF = jnp.bfloat16
F32 = jnp.float32
DP_TP = ("dp_0", "dp_1", "tp_0", "tp_1")
TP = ("tp_0", "tp_1")
DP = ("dp_0", "dp_1")
SCALE = (NOPE + ROPE) ** (-0.5)


def nt(a, b):
    return lax.dot_general(a, b, (((1,), (1,)), ((), ())), preferred_element_type=F32)


def nn(a, b):
    return lax.dot_general(a, b, (((1,), (0,)), ((), ())), preferred_element_type=F32)


def project(q_ref, u_ref, cos_ref, sin_ref, abs_ref, qr_ref, part, start, count):
    rows = pl.ds(start, count)

    def nope_pair(i):
        cols = pl.ds(i * 256, 256)
        both = nn(q_ref[rows, :], u_ref[:, 0:96, cols].reshape(QRANK, 256)).astype(BF)
        for j in range(2):
            own_cols = pl.ds(i * 256 + j * 128, 128)
            keys = u_ref[:, 96:128, own_cols].reshape(KVRANK, 128)
            abs_ref[i * 2 + j, rows, :] = nt(both[:, j * 128 : (j + 1) * 128], keys).astype(BF)

    lane = lax.broadcasted_iota(jnp.int32, (count, 128), 1)
    low = lax.rem(lane, 64) < 32

    def quad(i):
        nope_pair(2 * i)
        nope_pair(2 * i + 1)
        if i == 0:
            pe_cols = u_ref[:, 0:96, 1024:1280].reshape(QRANK, 256)
        else:
            tail = [u_ref[:, 96:128, 1024 + b * 128 : 1152 + b * 128] for b in range(3)]
            pe_cols = jnp.concatenate(
                [
                    u_ref[:, 0:96, 1280:1408].reshape(QRANK, 128),
                    jnp.concatenate(tail, axis=1).reshape(QRANK, 128),
                ],
                axis=1,
            )
        four = nn(q_ref[rows, :], pe_cols).astype(BF).astype(F32)
        for j in range(2):
            pe = four[:, j * 128 : (j + 1) * 128]
            other = jnp.where(low, pltpu.roll(pe, 96, 1), pltpu.roll(pe, 32, 1))
            rot = pe * cos_ref[rows, :] + other * sin_ref[rows, :]
            qr_ref[i * 4 + j * 2, rows, :] = rot.astype(BF)
            qr_ref[i * 4 + j * 2 + 1, rows, :] = pltpu.roll(rot, 64, 1).astype(BF)

    quad(part)


def scores_of(g, abs_ref, qr_ref, latn_ref, ropn_ref, lat, rop, sc_ref, scn_ref):
    rows = pl.ds(pl.multiple_of(g * 16, 16), 16)
    q = abs_ref[:, rows, :].reshape(128, KVRANK)
    qr = qr_ref[:, rows, 0:ROPE].reshape(128, ROPE)
    ropes = jnp.concatenate([rop[s] for s in range(4)], axis=1)
    wide = nt(q, lat[...].reshape(4 * CACHE, KVRANK)) + nn(qr, ropes)
    seq = lax.rem(lax.broadcasted_iota(jnp.int32, (128, CACHE), 0) // 4, 4)
    own = wide[:, 0:CACHE]
    for s in range(1, 4):
        own = jnp.where(seq == s, wide[:, s * CACHE : s * CACHE + CACHE], own)
    sc_ref[...] = own
    scn_ref[...] = nt(q, latn_ref[rows, :]) + nt(qr, ropn_ref[rows, :])


def attend(g, len_ref, latn_ref, lat, sc_ref, scn_ref, lo_ref):
    row = lax.broadcasted_iota(jnp.int32, (128, CACHE), 0)
    seq = lax.rem(row // 4, 4)
    limit = jnp.where(
        seq == 0,
        len_ref[g * 4],
        jnp.where(
            seq == 1, len_ref[g * 4 + 1], jnp.where(seq == 2, len_ref[g * 4 + 2], len_ref[g * 4 + 3])
        ),
    )
    at = lax.broadcasted_iota(jnp.int32, (128, CACHE), 1)
    sc = jnp.where(at < limit, sc_ref[...] * SCALE, -jnp.inf)
    nrow = lax.broadcasted_iota(jnp.int32, (128, 16), 0)
    ncol = lax.broadcasted_iota(jnp.int32, (128, 16), 1)
    fits = (lax.rem(nrow // 4, 4) == ncol // 4) & (lax.rem(ncol, 4) <= lax.rem(nrow, 4))
    scn = jnp.where(fits, scn_ref[...] * SCALE, -jnp.inf)
    top = jnp.maximum(
        jnp.max(sc, axis=1, keepdims=True), jnp.max(scn, axis=1, keepdims=True)
    )
    ex = jnp.exp(sc - top)
    exn = jnp.exp(scn - top)
    total = jnp.sum(ex, axis=1, keepdims=True) + jnp.sum(exn, axis=1, keepdims=True)
    share = 1.0 / total
    w = (ex * share).astype(BF)
    wn = (exn * share).astype(BF)
    zero = jnp.zeros_like(w)
    parts = jnp.concatenate([jnp.where(seq == s, w, zero) for s in range(4)], axis=1)
    rows = pl.ds(pl.multiple_of(g * 16, 16), 16)
    out = nn(parts, lat[...].reshape(4 * CACHE, KVRANK)) + nn(wn, latn_ref[rows, :])
    lo_ref[:, rows, :] = out.astype(BF).reshape(HL, 16, KVRANK)


MESH = pl.DeviceIdType.MESH
CHUNK = (64, 64, 64, 64)
FIRST = (0, 128, 256, 384)


def around(i, d):
    return lax.rem(i + d + 4, 4)


def layer_kernel(
    ropk_ref, asn_ref, lenv_ref, freq_ref, len_ref,
    uq_hbm, wk_hbm, wv_hbm, wo_hbm, q_hbm, latk_hbm, lat_hbm, rop_hbm,
    out_hbm, sel_hbm, norm_ref,
    uq_ref, wk_ref, wv_ref, wo_ref, q_ref, latk_ref, selk_ref, sel_ref, cos_ref, sin_ref,
    stage, packs, rp, opack, orp, u_ref, v_ref, wo_all, nsend, ntp, ny, nz,
    qs_ref, latn_ref, ropn_ref, abs_ref, qr_ref, lo_ref, lat_ref, rop_ref, sc0, scn0, sc1, scn1,
    ho_ref, hb_ref, ct_ref, r1_ref, rx_ref, fs_ref, ft_ref, ot_ref,
    in_sem, lat_sem, rop_sem, a2a_sem, o2a_sem, nt_sem, nyz_sem, ag_s, ag_r, uv_s, uv_r,
    oz_sem, od_sem, d2_s, d2_r, hy_s, hy_r, r1_s, r1_r, r2_s, r2_r, f_sem,
):
    z, y = lax.axis_index("dp_0"), lax.axis_index("dp_1")
    x, c = lax.axis_index("tp_0"), lax.axis_index("tp_1")
    t = x * 2 + c
    def copy_to(src, dst, ss, rs, **axes):
        names = {"z": "dp_0", "y": "dp_1", "x": "tp_0", "c": "tp_1"}
        return pltpu.make_async_remote_copy(
            src_ref=src, dst_ref=dst, send_sem=ss, recv_sem=rs,
            device_id={names[n]: v for n, v in axes.items()}, device_id_type=MESH,
        )

    def send(src, dst, ss, rs, **axes):
        copy_to(src, dst, ss, rs, **axes).start()

    def arrived(dst, rs):
        copy_to(dst, dst, rs, rs, c=1 - c).wait_recv()

    def left(src, ss):
        copy_to(src, src, ss, ss, c=1 - c).wait_send()

    barrier = pltpu.get_barrier_semaphore()

    def greet(**axes):
        names = {"z": "dp_0", "y": "dp_1", "x": "tp_0", "c": "tp_1"}
        pl.semaphore_signal(
            barrier, inc=1, device_id={names[n]: v for n, v in axes.items()}, device_id_type=MESH
        )

    for dt in range(1, 8):
        peer = lax.rem(t + dt, 8)
        greet(x=peer // 2, c=lax.rem(peer, 2))
    for d in range(1, 4):
        greet(z=around(z, d))
        greet(y=around(y, d))
        greet(y=around(y, d), c=1 - c)

    loads = []
    for n, (src, dst) in enumerate(
        (
            (uq_hbm, uq_ref), (wk_hbm, wk_ref), (wv_hbm, wv_ref), (wo_hbm, wo_ref), (q_hbm, q_ref),
            (latk_hbm, latk_ref),
        )
    ):
        loads.append(pltpu.make_async_copy(src, dst, in_sem.at[n]))
        loads[n].start()

    def fetch(g):
        slot = lax.rem(g, SLOTS)
        return (
            pltpu.make_async_copy(lat_hbm.at[pl.ds(g * 4, 4)], lat_ref.at[slot], lat_sem.at[slot]),
            pltpu.make_async_copy(rop_hbm.at[pl.ds(g * 4, 4)], rop_ref.at[slot], rop_sem.at[slot]),
        )

    def start(g):
        for made in fetch(g):
            made.start()

    def wait(g):
        for made in fetch(g):
            made.wait()

    for g in range(SLOTS - 1):
        start(g)

    lane12 = lax.broadcasted_iota(jnp.int32, (12, 128), 1)

    def fold(v):
        rows, cols = v.shape
        total = jnp.zeros((8, 128), F32)
        for i in range(rows // 8):
            for j in range(cols // 128):
                part = v[i * 8 : i * 8 + 8, j * 128 : j * 128 + 128]
                total = total + part * part
        return total

    def pack_one(p, squares):
        for i in range(4):
            v = uq_ref[:, pl.ds(pl.multiple_of(p * 1536 + i * 384, 128), 384)]
            v0, v1, v2 = v[:, 0:128], v[:, 128:256], v[:, 256:384]
            stage[p, 0:12, i * 256 : i * 256 + 128] = v0
            stage[p, 0:12, i * 256 + 128 : i * 256 + 256] = pltpu.roll(
                jnp.where(lane12 < 64, v2, v1), 64, 1
            )
            stage[p, 0:12, 1024 + i * 128 : 1152 + i * 128] = jnp.where(lane12 < 64, v1, v2)
            stage[p, i * 4 : i * 4 + 4, 1536:1792] = wv_ref[
                :, pl.ds(pl.multiple_of(p * 1024 + i * 256, 128), 256)
            ]
        stage[p, 12:16, 0:1024] = wk_ref[:, pl.ds(pl.multiple_of(p * 1024, 128), 1024)]
        stage[p, 12:16, 1024:1536] = jnp.zeros((4, 512), F32)
        whole = stage[p]
        packs[p] = whole.astype(BF)
        return squares + fold(whole)

    for n in range(3):
        loads[n].wait()
    squares = lax.fori_loop(0, 8, pack_one, jnp.zeros((8, 128), F32))
    pl.semaphore_wait(barrier, 16)
    for dt in (4, 5, 2, 3, 6, 7, 1):
        peer = lax.rem(t + dt, 8)
        send(
            packs.at[peer], rp.at[t], a2a_sem.at[0], a2a_sem.at[1], x=peer // 2, c=lax.rem(peer, 2)
        )
    rp[t] = packs[t]

    def pack_out(p, squares):
        v = wo_ref[:, pl.ds(pl.multiple_of(p * 1024, 128), 1024)]
        opack[p] = v.astype(BF)
        return squares + fold(v)

    loads[3].wait()
    squares = lax.fori_loop(0, 8, pack_out, squares)
    nsend[0] = squares
    ntp[t] = squares
    orp[t] = opack[t]

    row = lax.broadcasted_iota(jnp.int32, (TOK, TOK), 0)
    col = lax.broadcasted_iota(jnp.int32, (TOK, TOK), 1)
    spread = jnp.where(
        lax.broadcasted_iota(jnp.int32, (SEQS, TOK), 0)
        == lax.broadcasted_iota(jnp.int32, (SEQS, TOK), 1) // NEWTOK, 1.0, 0.0,
    ).astype(BF)
    slot_of = jnp.broadcast_to(asn_ref[...], (8, SEQS)).astype(F32)
    slot_by_token = nn(slot_of.astype(BF), spread)[0:1, :].astype(jnp.int32)
    slot_tiled = jnp.concatenate([asn_ref[...]] * NEWTOK, axis=1)
    selk_ref[0] = jnp.where(
        (slot_tiled == row // 4) & (col // SEQS == lax.rem(row, 4)), 1.0, 0.0
    ).astype(BF)
    same_token = lax.rem(row, 4) == lax.rem(col, 4)
    selk_ref[1] = jnp.where((slot_by_token == row // 4) & same_token, 1.0, 0.0).astype(BF)
    held = (
        (row // 256) * 256 + lax.rem(row // 64, 2) * 128 + lax.rem(row // 128, 2) * 64
        + lax.rem(row, 64)
    )
    back = jnp.where((slot_by_token == held // 4) & same_token, 1.0, 0.0).astype(BF)
    identity = jnp.where(row == col, 1.0, 0.0).astype(BF)
    sel_ref[...] = nt(identity, back).astype(BF)
    keep_sel = pltpu.make_async_copy(sel_ref, sel_hbm, in_sem.at[6])
    keep_out = pltpu.make_async_copy(ot_ref, out_hbm, in_sem.at[7])
    lengths_wide = jnp.broadcast_to(lenv_ref[...], (SEQS, SEQS)).astype(F32).astype(BF)

    def rotation(i, carry):
        rows = pl.ds(pl.multiple_of(i * 128, 128), 128)
        r = lax.broadcasted_iota(jnp.int32, (128, 128), 0) + i * 128
        lane = lax.broadcasted_iota(jnp.int32, (128, 128), 1)
        pick = jnp.where(r // 4 == lane, 1.0, 0.0).astype(BF)
        positions = nt(pick, lengths_wide) + lax.rem(r, 4).astype(F32)
        angles = positions * freq_ref[0:1, :]
        cos_ref[rows, :] = jnp.cos(angles)
        sine = jnp.sin(angles)
        sin_ref[rows, :] = jnp.where(lax.rem(lane, 64) < 32, -sine, sine)
        return carry

    arrived(rp.at[0:7], a2a_sem.at[1])
    big = rp[...].reshape(128, 1792)
    r = lax.broadcasted_iota(jnp.int32, (128, 128), 0)
    col = lax.broadcasted_iota(jnp.int32, (128, 128), 1)
    origin = jnp.where(
        r < 96, (r // 12) * 16 + lax.rem(r, 12), ((r - 96) // 4) * 16 + 12 + lax.rem(r - 96, 4)
    )
    order = jnp.where(col == origin, 1.0, 0.0).astype(BF)
    sorted_rows = nn(order, big[:, 0:1536]).astype(BF)
    r32 = lax.broadcasted_iota(jnp.int32, (32, 128), 0)
    col32 = lax.broadcasted_iota(jnp.int32, (32, 128), 1)
    uv_parts = []
    for i in range(4):
        pick = jnp.where(col32 == (r32 // 4) * 16 + i * 4 + lax.rem(r32, 4), 1.0, 0.0).astype(BF)
        uv_parts.append(nn(pick, big[:, 1536:1792]).astype(BF))
    me = z * 4 + y
    u_ref[me, 0:96] = sorted_rows[0:96, 0:1408]
    u_ref[me, 96:128, 0:1024] = sorted_rows[96:128, 0:1024]
    for i in range(3):
        u_ref[me, 96:128, 1024 + i * 128 : 1152 + i * 128] = sorted_rows[
            i * 32 : i * 32 + 32, 1408:1536
        ]
    v_ref[me] = jnp.concatenate(uv_parts, axis=1)

    def piece(ring, ia, ib, sub=None):
        if ring == 2:
            at = v_ref.at[ia * 4 + ib]
            return at if sub is None else at.at[:, pl.ds(sub * 512, 512)]
        rows = pl.ds(ring * 64, 64) if sub is None else pl.ds(ring * 64 + sub * 32, 32)
        return u_ref.at[ib * 4 + ia if ring == 0 else ia * 4 + ib, rows]

    def step(ring, along_first, to):
        first, second = ("y", "z") if ring == 0 else ("z", "y")
        return {first if along_first else second: to}

    where_a = [y, z, z]
    where_b = [z, y, y]

    def sent(ring):
        return ag_s.at[0] if ring < 2 else uv_s.at[0]

    def got(ring, n):
        if ring == 2:
            return uv_r.at[min(n, 12)]
        return ag_r.at[24 if n >= 12 else ring * 12 + n]

    offsets = (0, -1, 1, 2)

    def first_send(ring):
        a, b = where_a[ring], where_b[ring]
        for k, d in enumerate((1, -1)):
            ref = piece(ring, a, b)
            send(ref, ref, sent(ring), got(ring, k), **step(ring, True, around(a, d)))

    def first_forward(ring):
        a, b = where_a[ring], where_b[ring]
        for k, d in enumerate((1, -1)):
            arrived(piece(ring, around(a, -d), b), got(ring, k))
            ref = piece(ring, around(a, -d), b, k)
            send(ref, ref, sent(ring), got(ring, 2 + k), **step(ring, True, around(a, d)))

    def first_last(ring):
        a, b = where_a[ring], where_b[ring]
        for k in range(2):
            arrived(piece(ring, around(a, 2), b, k), got(ring, 2 + k))

    def second_send(ring, p):
        a, b = where_a[ring], where_b[ring]
        ia = around(a, offsets[p])
        for k, d in enumerate((1, -1)):
            ref = piece(ring, ia, b)
            send(ref, ref, sent(ring), got(ring, 4 + p * 2 + k), **step(ring, False, around(b, d)))

    def second_forward(ring, p):
        a, b = where_a[ring], where_b[ring]
        ia = around(a, offsets[p])
        for k, d in enumerate((1, -1)):
            arrived(piece(ring, ia, around(b, -d)), got(ring, 4 + p * 2 + k))
            ref = piece(ring, ia, around(b, -d), k)
            send(ref, ref, sent(ring), got(ring, 12), **step(ring, False, around(b, d)))

    for ring in range(2):
        first_send(ring)
    for ring in range(2):
        second_send(ring, 0)
    for dt in (4, 5, 2, 3, 6, 7, 1):
        peer = lax.rem(t + dt, 8)
        where = dict(x=peer // 2, c=lax.rem(peer, 2))
        send(nsend.at[0], ntp.at[t], nt_sem.at[0], nt_sem.at[1], **where)
        send(opack.at[peer], orp.at[t], o2a_sem.at[0], o2a_sem.at[1], **where)
    loads[4].wait()
    loads[5].wait()
    keep_sel.start()

    def move_q(i, carry):
        cols = pl.ds(pl.multiple_of(i * 256, 256), 256)
        qs_ref[:, cols] = nn(selk_ref[1], q_ref[:, :, cols].reshape(TOK, 256)).astype(BF)
        return carry

    lax.fori_loop(0, QRANK // 256, move_q, 0)
    for ring in range(2):
        first_forward(ring)
    for ring in range(2):
        second_send(ring, 1)
        second_send(ring, 2)
    arrived(ntp.at[0:7], nt_sem.at[1])
    line = ntp[0]
    for i in range(1, 8):
        line = line + ntp[i]
    latn_ref[...] = nn(selk_ref[1], latk_ref[...].reshape(TOK, KVRANK)).astype(BF)
    rope_rows = jnp.concatenate([ropk_ref[k] for k in range(4)], axis=1)
    ropn_ref[...] = nt(selk_ref[0], rope_rows).astype(BF)
    nsend[1] = line
    ny[y] = line
    for d in range(1, 4):
        send(nsend.at[1], ny.at[y], nyz_sem.at[0], nyz_sem.at[1], y=around(y, d))

    for ring in range(2):
        second_forward(ring, 0)
    for ring in range(2):
        first_last(ring)
        second_send(ring, 3)
    first_send(2)
    lax.fori_loop(0, 4, rotation, 0)
    arrived(ny.at[0:3], nyz_sem.at[1])
    plane = ((ny[0] + ny[1]) + ny[2]) + ny[3]
    nsend[2] = plane
    nz[z] = plane
    for d in range(1, 4):
        send(nsend.at[2], nz.at[z], nyz_sem.at[0], nyz_sem.at[2], z=around(z, d))
    for p in range(1, 3):
        for ring in range(2):
            second_forward(ring, p)
    arrived(orp.at[0:7], o2a_sem.at[1])
    wo_all[c, z] = jnp.concatenate([orp[i].astype(F32) for i in range(8)], axis=0).astype(BF)
    for ring in range(2):
        second_forward(ring, 3)
    first_forward(2)
    for p in range(3):
        second_send(2, p)
    send(wo_all.at[c, z], wo_all.at[c, z], od_sem.at[0], od_sem.at[1], c=1 - c)
    for later in range(2):
        for k, d in enumerate((1, -1)):
            part = wo_all.at[c, z, pl.ds((k ^ later) * 224, 224)]
            send(part, part, oz_sem.at[0], oz_sem.at[1 + later], z=around(z, d))
    first_last(2)
    second_send(2, 3)
    arrived(u_ref.at[0:4], ag_r.at[24])
    arrived(nz.at[0:3], nyz_sem.at[2])
    everything = ((nz[0] + nz[1]) + nz[2]) + nz[3]
    everything = jnp.sum(jnp.sum(everything, axis=1, keepdims=True), axis=0, keepdims=True)
    entries = HEADS * (NOPE + ROPE) + 2 * HEADS * NOPE + D
    norm_ref[0] = jnp.sqrt(everything / entries)[0, 0]

    def projected(part, start, count):
        project(qs_ref, u_ref, cos_ref, sin_ref, abs_ref, qr_ref, part, start, count)

    projected(0, 0, 144)
    second_forward(2, 0)
    projected(1, 0, 144)
    second_forward(2, 1)

    def project_rest(part):
        projected(part, 144, TOK - 144)

    def score(g, sc, scn):
        slot = lax.rem(g, SLOTS)
        scores_of(g, abs_ref, qr_ref, latn_ref, ropn_ref, lat_ref.at[slot], rop_ref.at[slot], sc, scn)

    def finish(g, sc, scn):
        attend(g, len_ref, latn_ref, lat_ref.at[lax.rem(g, SLOTS)], sc, scn, lo_ref)

    wait(0)
    score(0, sc0, scn0)

    def two(i):
        g = i * 2

        @pl.when(g + 3 < GROUPS)
        def _():
            start(g + 3)

        wait(g + 1)
        score(g + 1, sc1, scn1)
        finish(g, sc0, scn0)

        @pl.when(g + 4 < GROUPS)
        def _():
            start(g + 4)

        @pl.when(g + 2 < GROUPS)
        def _():
            wait(g + 2)

        score(jnp.minimum(g + 2, GROUPS - 1), sc0, scn0)
        finish(g + 1, sc1, scn1)

    def values_pass(p):
        second_forward(2, p)

    def values_ready():
        arrived(v_ref.at[0:4], uv_r.at[12])

    def out_pass():
        arrived(wo_all.at[c, z], oz_sem.at[1])
        for k, d in enumerate((1, -1)):
            part = wo_all.at[c, around(z, -d), pl.ds(k * 224, 224)]
            send(part, part, oz_sem.at[0], oz_sem.at[3], z=around(z, d))

    def out_near():
        arrived(wo_all.at[c, z], oz_sem.at[2])
        for d in (1, -1):
            near = wo_all.at[c, around(z, d)]
            send(near, near, od_sem.at[0], od_sem.at[1], c=1 - c)

    def out_far():
        far = wo_all.at[c, around(z, 2)]
        arrived(far, oz_sem.at[3])
        send(far, far, od_sem.at[0], od_sem.at[1], c=1 - c)

    def out_ready():
        arrived(wo_all.at[1 - c], od_sem.at[1])

    def head_values(j):
        n = CHUNK[j]
        rows = slice(FIRST[j], FIRST[j] + 2 * n)
        for h in range(HL):
            up = v_ref[:, :, h * 128 : h * 128 + 128].reshape(KVRANK, 128)
            both = nn(lo_ref[h, rows, :], up).astype(BF)
            for half in range(2):
                ho_ref[j, half, 0:n, h * 128 : h * 128 + 128] = both[half * n : half * n + n]
        hb_ref[j, y, c, 0:n] = ho_ref[j, c, 0:n]

    def heads_done(j):
        head_values(j)
        some = pl.ds(0, CHUNK[j])
        target = hb_ref.at[j, y, c, some]
        send(ho_ref.at[j, 1 - c, some], target, d2_s.at[0], d2_r.at[j], c=1 - c)
        for d in (1, -1):
            send(ho_ref.at[j, c, some], target, hy_s.at[0], hy_r.at[j, 0], y=around(y, d))

    def partner_half(j):
        ref = hb_ref.at[j, y, 1 - c, pl.ds(0, CHUNK[j])]
        arrived(ref, d2_r.at[j])
        for d in (1, -1):
            send(ref, ref, hy_s.at[0], hy_r.at[j, 0], y=around(y, d))

    def pass_on(j):
        some = pl.ds(0, CHUNK[j])
        arrived(hb_ref.at[j, pl.ds(0, 2), pl.ds(0, 2), some], hy_r.at[j, 0])
        for k, d in enumerate((1, -1)):
            ref = hb_ref.at[j, around(y, -d), k, some]
            send(ref, ref, hy_s.at[0], hy_r.at[j, 1], y=around(y, d))

    def multiply(j):
        n = CHUNK[j]
        lanes = pl.ds(0, 4 * n)
        arrived(hb_ref.at[j, around(y, 2), pl.ds(0, 2), pl.ds(0, n)], hy_r.at[j, 1])

        def block(m):
            zs = lax.rem(x + m, 4)
            tokens = jnp.concatenate(
                [hb_ref[j, :, k, 0:n].reshape(4 * n, 1024) for k in range(2)], axis=1
            )
            columns = jnp.concatenate([wo_all[k, zs] for k in range(2)], axis=1)
            ct_ref[j, zs, :, 0 : 4 * n] = nt(columns, tokens).astype(BF)

        block(2)
        for k, d in enumerate((1, -1)):
            send(
                ct_ref.at[j, around(x, 2), pl.ds(k * 224, 224), lanes], r1_ref.at[j, k, :, lanes],
                r1_s.at[0], r1_r.at[j], x=around(x, d),
            )

        def rest(m, carry):
            block(jnp.where(m == 0, 1, jnp.where(m == 1, 3, 0)))
            return carry

        lax.fori_loop(0, 3, rest, 0)
        for k, d in enumerate((1, -1)):
            part = pl.ds((1 - k) * 224, 224)
            send(
                ct_ref.at[j, around(x, d), part, lanes], rx_ref.at[j, k, part, lanes], r2_s.at[0],
                r2_r.at[j], x=around(x, d),
            )

    def add_far(j):
        n = 4 * CHUNK[j]
        lanes = pl.ds(0, n)
        arrived(r1_ref.at[j, :, :, lanes], r1_r.at[j])
        for k, d in enumerate((1, -1)):
            rows = slice(k * 224, k * 224 + 224)
            near = around(x, d)
            both = ct_ref[j, near, rows, 0:n].astype(F32) + r1_ref[j, k, :, 0:n].astype(F32)
            ct_ref[j, near, rows, 0:n] = both.astype(BF)
            part = pl.ds(k * 224, 224)
            send(
                ct_ref.at[j, near, part, lanes], rx_ref.at[j, k, part, lanes], r2_s.at[0],
                r2_r.at[j], x=near,
            )

    def collect(j):
        n = 4 * CHUNK[j]
        total = (
            ct_ref[j, x, :, 0:n].astype(F32)
            + rx_ref[j, 0, :, 0:n].astype(F32)
            + rx_ref[j, 1, :, 0:n].astype(F32)
        )
        if j % 2 == 0:
            fs_ref[...] = total
            return
        lane = lax.broadcasted_iota(jnp.int32, (448, 128), 1)
        for v in range(2):
            early = fs_ref[:, v * 128 : v * 128 + 128]
            late = total[:, v * 128 : v * 128 + 128]
            at = j // 2 * 4 + 2 * v
            ft_ref[at] = jnp.where(lane < 64, early, pltpu.roll(late, 64, 1)).astype(BF)
            ft_ref[at + 1] = jnp.where(lane < 64, pltpu.roll(early, 64, 1), late).astype(BF)

    here = y // 2 == c

    def add_near(j):
        arrived(rx_ref.at[j, :, :, pl.ds(0, 4 * CHUNK[j])], r2_r.at[j])
        collect(j)
        if j % 2 == 0:
            return
        pair = j // 2
        target = ot_ref.at[
            pl.ds(pl.multiple_of(lax.rem(y, 2) * 448, 448), 448),
            pl.ds(pl.multiple_of((pair * 2 + c) * 128, 128), 128),
        ]
        for d in (2, 1, 3):
            to = around(y, d)
            send(ft_ref.at[pair * 4 + to], target, f_sem.at[0], f_sem.at[1], y=to, c=y // 2)

        @pl.when(here)
        def _():
            target[...] = ft_ref[pair * 4 + y]

        @pl.when(jnp.logical_not(here))
        def _():
            send(ft_ref.at[pair * 4 + y], target, f_sem.at[2], f_sem.at[1], c=1 - c)

    plan = {
        0: [(values_pass, 2)],
        1: [(values_pass, 3)],
        3: [
            (values_ready,), (heads_done, 0), (out_pass,), (project_rest, 0), (partner_half, 0),
            (project_rest, 1),
        ],
        4: [(pass_on, 0)],
        6: [(out_near,)],
        7: [(heads_done, 1)],
        8: [(partner_half, 1)],
        10: [(out_far,)],
        11: [(pass_on, 1), (heads_done, 2), (out_ready,), (multiply, 0)],
        12: [(partner_half, 2)],
        13: [(add_far, 0)],
        15: [(pass_on, 2), (heads_done, 3)],
        16: [(add_near, 0), (partner_half, 3)],
        17: [(multiply, 1), (multiply, 2)],
        18: [(add_far, 1), (pass_on, 3), (add_far, 2)],
        19: [(multiply, 3), (add_near, 1), (add_near, 2), (add_far, 3), (add_near, 3)],
    }

    def run(events):
        for event, *which in events:
            event(*which)

    def together(i, carry):
        two(i)
        for slot in range(16):
            if slot in plan:

                @pl.when(i == slot)
                def _():
                    run(plan[slot])

        return carry

    lax.fori_loop(0, 16, together, 0)
    for slot in range(16, 20):
        run(plan[slot])

    @pl.when(here)
    def _():
        arrived(ft_ref.at[0:6], f_sem.at[1])

    @pl.when(jnp.logical_not(here))
    def _():
        arrived(ft_ref.at[0:8], f_sem.at[1])

    keep_out.start()
    left(packs.at[0:7], a2a_sem.at[0])
    left(opack.at[0:7], o2a_sem.at[0])
    left(ntp.at[0:7], nt_sem.at[0])
    left(ntp.at[0:6], nyz_sem.at[0])
    left(u_ref.at[0:15], ag_s.at[0])
    left(v_ref.at[0:15], uv_s.at[0])
    left(wo_all.at[0, 0:3], oz_sem.at[0])
    left(wo_all.at[0], od_sem.at[0])
    left(ho_ref.at[0:2], d2_s.at[0])
    left(hb_ref.at[0:3], hy_s.at[0])
    left(ct_ref.at[0], r1_s.at[0])
    left(ct_ref.at[0:2], r2_s.at[0])
    left(ft_ref.at[0:6], f_sem.at[0])

    @pl.when(jnp.logical_not(here))
    def _():
        left(ft_ref.at[0:2], f_sem.at[2])

    keep_sel.wait()
    keep_out.wait()


def layer(uq, wk, wv, wo, q, latk, ropk, slot_of, lengths, frequency, cache_latent, cache_rope):
    vmem = pl.BlockSpec(memory_space=pltpu.VMEM)
    smem = pl.BlockSpec(memory_space=pltpu.SMEM)
    hbm = pl.BlockSpec(memory_space=pl.ANY)
    dma = pltpu.SemaphoreType.DMA
    scratch = [
        ((12, 12288), F32), ((4, 8192), F32), ((4, 8192), F32), ((56, 8192), F32),
        ((SEQS, 4, QRANK), BF), ((SEQS, 4, KVRANK), BF), ((2, TOK, TOK), BF), ((TOK, TOK), BF),
        ((TOK, 128), F32), ((TOK, 128), F32),
        ((8, 16, 1792), F32), ((8, 16, 1792), BF), ((8, 16, 1792), BF),
        ((8, 56, 1024), BF), ((8, 56, 1024), BF),
        ((16, 128, 1408), BF), ((16, 32, 1024), BF), ((2, 4, 448, 1024), BF),
        ((3, 8, 128), F32), ((8, 8, 128), F32), ((4, 8, 128), F32), ((4, 8, 128), F32),
        ((TOK, QRANK), BF), ((TOK, KVRANK), BF), ((TOK, ROPE), BF),
        ((HL, TOK, KVRANK), BF), ((HL, TOK, 128), BF), ((HL, TOK, KVRANK), BF),
        ((SLOTS, 4, CACHE, KVRANK), BF), ((SLOTS, 4, ROPE, CACHE), BF),
        ((128, CACHE), F32), ((128, 16), F32), ((128, CACHE), F32), ((128, 16), F32),
        ((4, 2, 64, 1024), BF), ((4, 4, 2, 64, 1024), BF),
        ((4, 4, 448, 256), BF), ((4, 2, 224, 256), BF), ((4, 2, 448, 256), BF),
        ((448, 256), F32), ((8, 448, 128), BF), ((896, TOK), BF),
    ]
    counts = [
        (8,), (SLOTS,), (SLOTS,), (2,), (2,), (2,), (3,), (1,), (25,), (1,), (13,),
        (4,), (2,), (1,), (4,), (1,), (4, 2), (1,), (4,), (1,), (4,), (3,),
    ]
    return pl.pallas_call(
        layer_kernel,
        out_shape=(
            jax.ShapeDtypeStruct((896, TOK), BF), jax.ShapeDtypeStruct((TOK, TOK), BF),
            jax.ShapeDtypeStruct((1,), F32),
        ),
        in_specs=[vmem] * 4 + [smem] + [hbm] * 8,
        out_specs=(hbm, hbm, smem),
        scratch_shapes=[pltpu.VMEM(s, d) for s, d in scratch] + [dma(n) for n in counts],
        compiler_params=pltpu.CompilerParams(
            vmem_limit_bytes=67043328, collective_id=0, has_side_effects=True
        ),
        name="layer",
    )(
        ropk, slot_of, lengths.reshape(1, SEQS), frequency, lengths,
        uq, wk, wv, wo, q, latk, cache_latent, cache_rope,
    )


def shards(q_latent, new_latent, new_rope, cache_latent, cache_rope, lengths, assignment, w_uq, w_uk, w_uv, w_o):
    half = ROPE // 2
    frequency = 10000.0 ** (-np.arange(half, dtype=np.float32) / half)
    frequency = np.broadcast_to(np.tile(frequency, 4)[None, :], (8, 128)).astype(np.float32)
    held, sel, norm = layer(
        w_uq, w_uk, w_uv, w_o.T, q_latent, new_latent, new_rope.transpose(1, 2, 0), assignment,
        lengths, jnp.asarray(frequency), cache_latent, cache_rope,
    )
    out = nt(sel, held).astype(BF).reshape(SEQS, NEWTOK, 896)
    return out, norm


def solution(mesh):
    split = Mesh(mesh.devices.reshape(4, 4, 4, 2), ("dp_0", "dp_1", "tp_0", "tp_1"))
    dp, tp = ("dp_0", "dp_1"), ("tp_0", "tp_1")
    placed = (
        P(dp, None, None), P(dp, None, None), P(dp, None, None), P(dp, None, None), P(dp, None, None),
        P(dp), P(dp, None), P(dp + tp, None), P(dp + tp, None), P(dp + tp, None), P(None, dp + tp),
    )
    return jax.shard_map(
        shards, mesh=split, in_specs=placed, out_specs=(P(dp, None, tp), P()), check_vma=False
    )
```

```python
import jax
import jax.numpy as jnp
import numpy as np
from jax import lax
from jax.experimental import pallas as pl
from jax.experimental.pallas import tpu as pltpu
from jax.sharding import Mesh
from jax.sharding import PartitionSpec as P

D = 7168
QRANK = 1536
KVRANK = 512
NOPE = 128
ROPE = 64
VDIM = 128
HEADS = 64
NEWTOK = 4
CACHE = 256
SEQS = 128
TOK = SEQS * NEWTOK
HL = 8
GROUPS = SEQS // 4
SLOTS = 4
BF = jnp.bfloat16
F32 = jnp.float32
DP_TP = ("dp_0", "dp_1", "tp_0", "tp_1")
TP = ("tp_0", "tp_1")
DP = ("dp_0", "dp_1")
SCALE = (NOPE + ROPE) ** (-0.5)


def nt(a, b):
    return lax.dot_general(a, b, (((1,), (1,)), ((), ())), preferred_element_type=F32)


def nn(a, b):
    return lax.dot_general(a, b, (((1,), (0,)), ((), ())), preferred_element_type=F32)


def project(q_ref, u_ref, cos_ref, sin_ref, abs_ref, qr_ref, part, start, count):
    rows = pl.ds(start, count)

    def nope_pair(i):
        cols = pl.ds(i * 256, 256)
        both = nn(q_ref[rows, :], u_ref[:, 0:96, cols].reshape(QRANK, 256)).astype(BF)
        for j in range(2):
            own_cols = pl.ds(i * 256 + j * 128, 128)
            keys = u_ref[:, 96:128, own_cols].reshape(KVRANK, 128)
            abs_ref[i * 2 + j, rows, :] = nt(both[:, j * 128 : (j + 1) * 128], keys).astype(BF)

    lane = lax.broadcasted_iota(jnp.int32, (count, 128), 1)
    low = lax.rem(lane, 64) < 32

    def quad(i):
        nope_pair(2 * i)
        nope_pair(2 * i + 1)
        if i == 0:
            pe_cols = u_ref[:, 0:96, 1024:1280].reshape(QRANK, 256)
        else:
            tail = [u_ref[:, 96:128, 1024 + b * 128 : 1152 + b * 128] for b in range(3)]
            pe_cols = jnp.concatenate(
                [
                    u_ref[:, 0:96, 1280:1408].reshape(QRANK, 128),
                    jnp.concatenate(tail, axis=1).reshape(QRANK, 128),
                ],
                axis=1,
            )
        four = nn(q_ref[rows, :], pe_cols).astype(BF).astype(F32)
        for j in range(2):
            pe = four[:, j * 128 : (j + 1) * 128]
            other = jnp.where(low, pltpu.roll(pe, 96, 1), pltpu.roll(pe, 32, 1))
            rot = pe * cos_ref[rows, :] + other * sin_ref[rows, :]
            qr_ref[i * 4 + j * 2, rows, :] = rot.astype(BF)
            qr_ref[i * 4 + j * 2 + 1, rows, :] = pltpu.roll(rot, 64, 1).astype(BF)

    quad(part)


def scores_of(g, abs_ref, qr_ref, latn_ref, ropn_ref, lat, rop, sc_ref, scn_ref):
    rows = pl.ds(pl.multiple_of(g * 16, 16), 16)
    q = abs_ref[:, rows, :].reshape(128, KVRANK)
    qr = qr_ref[:, rows, 0:ROPE].reshape(128, ROPE)
    ropes = jnp.concatenate([rop[s] for s in range(4)], axis=1)
    wide = nt(q, lat[...].reshape(4 * CACHE, KVRANK)) + nn(qr, ropes)
    seq = lax.rem(lax.broadcasted_iota(jnp.int32, (128, CACHE), 0) // 4, 4)
    own = wide[:, 0:CACHE]
    for s in range(1, 4):
        own = jnp.where(seq == s, wide[:, s * CACHE : s * CACHE + CACHE], own)
    sc_ref[...] = own
    scn_ref[...] = nt(q, latn_ref[rows, :]) + nt(qr, ropn_ref[rows, :])


def attend(g, len_ref, latn_ref, lat, sc_ref, scn_ref, lo_ref):
    row = lax.broadcasted_iota(jnp.int32, (128, CACHE), 0)
    seq = lax.rem(row // 4, 4)
    limit = jnp.where(
        seq == 0,
        len_ref[g * 4],
        jnp.where(
            seq == 1, len_ref[g * 4 + 1], jnp.where(seq == 2, len_ref[g * 4 + 2], len_ref[g * 4 + 3])
        ),
    )
    at = lax.broadcasted_iota(jnp.int32, (128, CACHE), 1)
    sc = jnp.where(at < limit, sc_ref[...] * SCALE, -jnp.inf)
    nrow = lax.broadcasted_iota(jnp.int32, (128, 16), 0)
    ncol = lax.broadcasted_iota(jnp.int32, (128, 16), 1)
    fits = (lax.rem(nrow // 4, 4) == ncol // 4) & (lax.rem(ncol, 4) <= lax.rem(nrow, 4))
    scn = jnp.where(fits, scn_ref[...] * SCALE, -jnp.inf)
    top = jnp.maximum(
        jnp.max(sc, axis=1, keepdims=True), jnp.max(scn, axis=1, keepdims=True)
    )
    ex = jnp.exp(sc - top)
    exn = jnp.exp(scn - top)
    total = jnp.sum(ex, axis=1, keepdims=True) + jnp.sum(exn, axis=1, keepdims=True)
    share = 1.0 / total
    w = (ex * share).astype(BF)
    wn = (exn * share).astype(BF)
    zero = jnp.zeros_like(w)
    parts = jnp.concatenate([jnp.where(seq == s, w, zero) for s in range(4)], axis=1)
    rows = pl.ds(pl.multiple_of(g * 16, 16), 16)
    out = nn(parts, lat[...].reshape(4 * CACHE, KVRANK)) + nn(wn, latn_ref[rows, :])
    lo_ref[:, rows, :] = out.astype(BF).reshape(HL, 16, KVRANK)


MESH = pl.DeviceIdType.MESH
CHUNK = (64, 64, 64, 64)
FIRST = (0, 128, 256, 384)


def around(i, d):
    return lax.rem(i + d + 4, 4)


def layer_kernel(
    ropk_ref, asn_ref, lenv_ref, freq_ref, len_ref,
    uq_hbm, wk_hbm, wv_hbm, wo_hbm, q_hbm, latk_hbm, lat_hbm, rop_hbm,
    out_hbm, sel_hbm, norm_ref,
    uq_ref, wk_ref, wv_ref, wo_ref, q_ref, latk_ref, selk_ref, sel_ref, cos_ref, sin_ref,
    stage, packs, rp, opack, orp, u_ref, v_ref, wo_all, nsend, ntp, ny, nz,
    qs_ref, latn_ref, ropn_ref, abs_ref, qr_ref, lo_ref, lat_ref, rop_ref, sc0, scn0, sc1, scn1,
    ho_ref, hb_ref, ct_ref, r1_ref, rx_ref, fs_ref, ft_ref, ot_ref,
    in_sem, lat_sem, rop_sem, a2a_sem, o2a_sem, nt_sem, nyz_sem, ag_s, ag_r, uv_s, uv_r,
    oz_sem, od_sem, d2_s, d2_r, hy_s, hy_r, r1_s, r1_r, r2_s, r2_r, f_sem,
):
    z, y = lax.axis_index("dp_0"), lax.axis_index("dp_1")
    x, c = lax.axis_index("tp_0"), lax.axis_index("tp_1")
    t = x * 2 + c
    def copy_to(src, dst, ss, rs, **axes):
        names = {"z": "dp_0", "y": "dp_1", "x": "tp_0", "c": "tp_1"}
        return pltpu.make_async_remote_copy(
            src_ref=src, dst_ref=dst, send_sem=ss, recv_sem=rs,
            device_id={names[n]: v for n, v in axes.items()}, device_id_type=MESH,
        )

    def send(src, dst, ss, rs, **axes):
        copy_to(src, dst, ss, rs, **axes).start()

    def arrived(dst, rs):
        copy_to(dst, dst, rs, rs, c=1 - c).wait_recv()

    def left(src, ss):
        copy_to(src, src, ss, ss, c=1 - c).wait_send()

    barrier = pltpu.get_barrier_semaphore()

    def greet(**axes):
        names = {"z": "dp_0", "y": "dp_1", "x": "tp_0", "c": "tp_1"}
        pl.semaphore_signal(
            barrier, inc=1, device_id={names[n]: v for n, v in axes.items()}, device_id_type=MESH
        )

    for dt in range(1, 8):
        peer = lax.rem(t + dt, 8)
        greet(x=peer // 2, c=lax.rem(peer, 2))
    for d in range(1, 4):
        greet(z=around(z, d))
        greet(y=around(y, d))
        greet(y=around(y, d), c=1 - c)

    loads = []
    for n, (src, dst) in enumerate(
        (
            (uq_hbm, uq_ref), (wk_hbm, wk_ref), (wv_hbm, wv_ref), (wo_hbm, wo_ref), (q_hbm, q_ref),
            (latk_hbm, latk_ref),
        )
    ):
        loads.append(pltpu.make_async_copy(src, dst, in_sem.at[n]))
        loads[n].start()

    def fetch(g):
        slot = lax.rem(g, SLOTS)
        return (
            pltpu.make_async_copy(lat_hbm.at[pl.ds(g * 4, 4)], lat_ref.at[slot], lat_sem.at[slot]),
            pltpu.make_async_copy(rop_hbm.at[pl.ds(g * 4, 4)], rop_ref.at[slot], rop_sem.at[slot]),
        )

    def start(g):
        for made in fetch(g):
            made.start()

    def wait(g):
        for made in fetch(g):
            made.wait()

    for g in range(SLOTS - 1):
        start(g)

    lane12 = lax.broadcasted_iota(jnp.int32, (12, 128), 1)

    def fold(v):
        rows, cols = v.shape
        total = jnp.zeros((8, 128), F32)
        for i in range(rows // 8):
            for j in range(cols // 128):
                part = v[i * 8 : i * 8 + 8, j * 128 : j * 128 + 128]
                total = total + part * part
        return total

    def pack_one(p, squares):
        for i in range(4):
            v = uq_ref[:, pl.ds(pl.multiple_of(p * 1536 + i * 384, 128), 384)]
            v0, v1, v2 = v[:, 0:128], v[:, 128:256], v[:, 256:384]
            stage[p, 0:12, i * 256 : i * 256 + 128] = v0
            stage[p, 0:12, i * 256 + 128 : i * 256 + 256] = pltpu.roll(
                jnp.where(lane12 < 64, v2, v1), 64, 1
            )
            stage[p, 0:12, 1024 + i * 128 : 1152 + i * 128] = jnp.where(lane12 < 64, v1, v2)
            stage[p, i * 4 : i * 4 + 4, 1536:1792] = wv_ref[
                :, pl.ds(pl.multiple_of(p * 1024 + i * 256, 128), 256)
            ]
        stage[p, 12:16, 0:1024] = wk_ref[:, pl.ds(pl.multiple_of(p * 1024, 128), 1024)]
        stage[p, 12:16, 1024:1536] = jnp.zeros((4, 512), F32)
        whole = stage[p]
        packs[p] = whole.astype(BF)
        return squares + fold(whole)

    for n in range(3):
        loads[n].wait()
    squares = lax.fori_loop(0, 8, pack_one, jnp.zeros((8, 128), F32))
    pl.semaphore_wait(barrier, 16)
    for dt in (4, 5, 2, 3, 6, 7, 1):
        peer = lax.rem(t + dt, 8)
        send(
            packs.at[peer], rp.at[t], a2a_sem.at[0], a2a_sem.at[1], x=peer // 2, c=lax.rem(peer, 2)
        )
    rp[t] = packs[t]

    def pack_out(p, squares):
        v = wo_ref[:, pl.ds(pl.multiple_of(p * 1024, 128), 1024)]
        opack[p] = v.astype(BF)
        return squares + fold(v)

    loads[3].wait()
    squares = lax.fori_loop(0, 8, pack_out, squares)
    nsend[0] = squares
    ntp[t] = squares
    orp[t] = opack[t]

    row = lax.broadcasted_iota(jnp.int32, (TOK, TOK), 0)
    col = lax.broadcasted_iota(jnp.int32, (TOK, TOK), 1)
    spread = jnp.where(
        lax.broadcasted_iota(jnp.int32, (SEQS, TOK), 0)
        == lax.broadcasted_iota(jnp.int32, (SEQS, TOK), 1) // NEWTOK, 1.0, 0.0,
    ).astype(BF)
    slot_of = jnp.broadcast_to(asn_ref[...], (8, SEQS)).astype(F32)
    slot_by_token = nn(slot_of.astype(BF), spread)[0:1, :].astype(jnp.int32)
    slot_tiled = jnp.concatenate([asn_ref[...]] * NEWTOK, axis=1)
    selk_ref[0] = jnp.where(
        (slot_tiled == row // 4) & (col // SEQS == lax.rem(row, 4)), 1.0, 0.0
    ).astype(BF)
    same_token = lax.rem(row, 4) == lax.rem(col, 4)
    selk_ref[1] = jnp.where((slot_by_token == row // 4) & same_token, 1.0, 0.0).astype(BF)
    held = (
        (row // 256) * 256 + lax.rem(row // 64, 2) * 128 + lax.rem(row // 128, 2) * 64
        + lax.rem(row, 64)
    )
    back = jnp.where((slot_by_token == held // 4) & same_token, 1.0, 0.0).astype(BF)
    identity = jnp.where(row == col, 1.0, 0.0).astype(BF)
    sel_ref[...] = nt(identity, back).astype(BF)
    keep_sel = pltpu.make_async_copy(sel_ref, sel_hbm, in_sem.at[6])
    keep_out = pltpu.make_async_copy(ot_ref, out_hbm, in_sem.at[7])
    lengths_wide = jnp.broadcast_to(lenv_ref[...], (SEQS, SEQS)).astype(F32).astype(BF)

    def rotation(i, carry):
        rows = pl.ds(pl.multiple_of(i * 128, 128), 128)
        r = lax.broadcasted_iota(jnp.int32, (128, 128), 0) + i * 128
        lane = lax.broadcasted_iota(jnp.int32, (128, 128), 1)
        pick = jnp.where(r // 4 == lane, 1.0, 0.0).astype(BF)
        positions = nt(pick, lengths_wide) + lax.rem(r, 4).astype(F32)
        angles = positions * freq_ref[0:1, :]
        cos_ref[rows, :] = jnp.cos(angles)
        sine = jnp.sin(angles)
        sin_ref[rows, :] = jnp.where(lax.rem(lane, 64) < 32, -sine, sine)
        return carry

    arrived(rp.at[0:7], a2a_sem.at[1])
    big = rp[...].reshape(128, 1792)
    r = lax.broadcasted_iota(jnp.int32, (128, 128), 0)
    col = lax.broadcasted_iota(jnp.int32, (128, 128), 1)
    origin = jnp.where(
        r < 96, (r // 12) * 16 + lax.rem(r, 12), ((r - 96) // 4) * 16 + 12 + lax.rem(r - 96, 4)
    )
    order = jnp.where(col == origin, 1.0, 0.0).astype(BF)
    sorted_rows = nn(order, big[:, 0:1536]).astype(BF)
    r32 = lax.broadcasted_iota(jnp.int32, (32, 128), 0)
    col32 = lax.broadcasted_iota(jnp.int32, (32, 128), 1)
    uv_parts = []
    for i in range(4):
        pick = jnp.where(col32 == (r32 // 4) * 16 + i * 4 + lax.rem(r32, 4), 1.0, 0.0).astype(BF)
        uv_parts.append(nn(pick, big[:, 1536:1792]).astype(BF))
    me = z * 4 + y
    u_ref[me, 0:96] = sorted_rows[0:96, 0:1408]
    u_ref[me, 96:128, 0:1024] = sorted_rows[96:128, 0:1024]
    for i in range(3):
        u_ref[me, 96:128, 1024 + i * 128 : 1152 + i * 128] = sorted_rows[
            i * 32 : i * 32 + 32, 1408:1536
        ]
    v_ref[me] = jnp.concatenate(uv_parts, axis=1)

    def piece(ring, ia, ib, sub=None):
        if ring == 2:
            at = v_ref.at[ia * 4 + ib]
            return at if sub is None else at.at[:, pl.ds(sub * 512, 512)]
        rows = pl.ds(ring * 64, 64) if sub is None else pl.ds(ring * 64 + sub * 32, 32)
        return u_ref.at[ib * 4 + ia if ring == 0 else ia * 4 + ib, rows]

    def step(ring, along_first, to):
        first, second = ("y", "z") if ring == 0 else ("z", "y")
        return {first if along_first else second: to}

    where_a = [y, z, z]
    where_b = [z, y, y]

    def sent(ring):
        return ag_s.at[0] if ring < 2 else uv_s.at[0]

    def got(ring, n):
        if ring == 2:
            return uv_r.at[min(n, 12)]
        return ag_r.at[24 if n >= 12 else ring * 12 + n]

    offsets = (0, -1, 1, 2)

    def first_send(ring):
        a, b = where_a[ring], where_b[ring]
        for k, d in enumerate((1, -1)):
            ref = piece(ring, a, b)
            send(ref, ref, sent(ring), got(ring, k), **step(ring, True, around(a, d)))

    def first_forward(ring):
        a, b = where_a[ring], where_b[ring]
        for k, d in enumerate((1, -1)):
            arrived(piece(ring, around(a, -d), b), got(ring, k))
            ref = piece(ring, around(a, -d), b, k)
            send(ref, ref, sent(ring), got(ring, 2 + k), **step(ring, True, around(a, d)))

    def first_last(ring):
        a, b = where_a[ring], where_b[ring]
        for k in range(2):
            arrived(piece(ring, around(a, 2), b, k), got(ring, 2 + k))

    def second_send(ring, p):
        a, b = where_a[ring], where_b[ring]
        ia = around(a, offsets[p])
        for k, d in enumerate((1, -1)):
            ref = piece(ring, ia, b)
            send(ref, ref, sent(ring), got(ring, 4 + p * 2 + k), **step(ring, False, around(b, d)))

    def second_forward(ring, p):
        a, b = where_a[ring], where_b[ring]
        ia = around(a, offsets[p])
        for k, d in enumerate((1, -1)):
            arrived(piece(ring, ia, around(b, -d)), got(ring, 4 + p * 2 + k))
            ref = piece(ring, ia, around(b, -d), k)
            send(ref, ref, sent(ring), got(ring, 12), **step(ring, False, around(b, d)))

    for ring in range(2):
        first_send(ring)
    for ring in range(2):
        second_send(ring, 0)
    for dt in (4, 5, 2, 3, 6, 7, 1):
        peer = lax.rem(t + dt, 8)
        where = dict(x=peer // 2, c=lax.rem(peer, 2))
        send(nsend.at[0], ntp.at[t], nt_sem.at[0], nt_sem.at[1], **where)
        send(opack.at[peer], orp.at[t], o2a_sem.at[0], o2a_sem.at[1], **where)
    loads[4].wait()
    loads[5].wait()
    keep_sel.start()

    def move_q(i, carry):
        cols = pl.ds(pl.multiple_of(i * 256, 256), 256)
        qs_ref[:, cols] = nn(selk_ref[1], q_ref[:, :, cols].reshape(TOK, 256)).astype(BF)
        return carry

    lax.fori_loop(0, QRANK // 256, move_q, 0)
    for ring in range(2):
        first_forward(ring)
    for ring in range(2):
        second_send(ring, 1)
        second_send(ring, 2)
    arrived(ntp.at[0:7], nt_sem.at[1])
    line = ntp[0]
    for i in range(1, 8):
        line = line + ntp[i]
    latn_ref[...] = nn(selk_ref[1], latk_ref[...].reshape(TOK, KVRANK)).astype(BF)
    rope_rows = jnp.concatenate([ropk_ref[k] for k in range(4)], axis=1)
    ropn_ref[...] = nt(selk_ref[0], rope_rows).astype(BF)
    nsend[1] = line
    ny[y] = line
    for d in range(1, 4):
        send(nsend.at[1], ny.at[y], nyz_sem.at[0], nyz_sem.at[1], y=around(y, d))

    for ring in range(2):
        second_forward(ring, 0)
    for ring in range(2):
        first_last(ring)
        second_send(ring, 3)
    first_send(2)
    lax.fori_loop(0, 4, rotation, 0)
    arrived(ny.at[0:3], nyz_sem.at[1])
    plane = ((ny[0] + ny[1]) + ny[2]) + ny[3]
    nsend[2] = plane
    nz[z] = plane
    for d in range(1, 4):
        send(nsend.at[2], nz.at[z], nyz_sem.at[0], nyz_sem.at[2], z=around(z, d))
    for p in range(1, 3):
        for ring in range(2):
            second_forward(ring, p)
    arrived(orp.at[0:7], o2a_sem.at[1])
    wo_all[c, z] = jnp.concatenate([orp[i].astype(F32) for i in range(8)], axis=0).astype(BF)
    for ring in range(2):
        second_forward(ring, 3)
    first_forward(2)
    for p in range(3):
        second_send(2, p)
    send(wo_all.at[c, z], wo_all.at[c, z], od_sem.at[0], od_sem.at[1], c=1 - c)
    for later in range(2):
        for k, d in enumerate((1, -1)):
            part = wo_all.at[c, z, pl.ds((k ^ later) * 224, 224)]
            send(part, part, oz_sem.at[0], oz_sem.at[1 + later], z=around(z, d))
    first_last(2)
    second_send(2, 3)
    arrived(u_ref.at[0:4], ag_r.at[24])
    arrived(nz.at[0:3], nyz_sem.at[2])
    everything = ((nz[0] + nz[1]) + nz[2]) + nz[3]
    everything = jnp.sum(jnp.sum(everything, axis=1, keepdims=True), axis=0, keepdims=True)
    entries = HEADS * (NOPE + ROPE) + 2 * HEADS * NOPE + D
    norm_ref[0] = jnp.sqrt(everything / entries)[0, 0]

    def projected(part, start, count):
        project(qs_ref, u_ref, cos_ref, sin_ref, abs_ref, qr_ref, part, start, count)

    projected(0, 0, 144)
    second_forward(2, 0)
    projected(1, 0, 144)
    second_forward(2, 1)

    def project_rest(part):
        projected(part, 144, TOK - 144)

    def score(g, sc, scn):
        slot = lax.rem(g, SLOTS)
        scores_of(g, abs_ref, qr_ref, latn_ref, ropn_ref, lat_ref.at[slot], rop_ref.at[slot], sc, scn)

    def finish(g, sc, scn):
        attend(g, len_ref, latn_ref, lat_ref.at[lax.rem(g, SLOTS)], sc, scn, lo_ref)

    wait(0)
    score(0, sc0, scn0)

    def two(i):
        g = i * 2

        @pl.when(g + 3 < GROUPS)
        def _():
            start(g + 3)

        wait(g + 1)
        score(g + 1, sc1, scn1)
        finish(g, sc0, scn0)

        @pl.when(g + 4 < GROUPS)
        def _():
            start(g + 4)

        @pl.when(g + 2 < GROUPS)
        def _():
            wait(g + 2)

        score(jnp.minimum(g + 2, GROUPS - 1), sc0, scn0)
        finish(g + 1, sc1, scn1)

    def values_pass(p):
        second_forward(2, p)

    def values_ready():
        arrived(v_ref.at[0:4], uv_r.at[12])

    def out_pass():
        arrived(wo_all.at[c, z], oz_sem.at[1])
        for k, d in enumerate((1, -1)):
            part = wo_all.at[c, around(z, -d), pl.ds(k * 224, 224)]
            send(part, part, oz_sem.at[0], oz_sem.at[3], z=around(z, d))

    def out_near():
        arrived(wo_all.at[c, z], oz_sem.at[2])
        for d in (1, -1):
            near = wo_all.at[c, around(z, d)]
            send(near, near, od_sem.at[0], od_sem.at[1], c=1 - c)

    def out_far():
        far = wo_all.at[c, around(z, 2)]
        arrived(far, oz_sem.at[3])
        send(far, far, od_sem.at[0], od_sem.at[1], c=1 - c)

    def out_ready():
        arrived(wo_all.at[1 - c], od_sem.at[1])

    def head_values(j):
        n = CHUNK[j]
        rows = slice(FIRST[j], FIRST[j] + 2 * n)
        for h in range(HL):
            up = v_ref[:, :, h * 128 : h * 128 + 128].reshape(KVRANK, 128)
            both = nn(lo_ref[h, rows, :], up).astype(BF)
            for half in range(2):
                ho_ref[j, half, 0:n, h * 128 : h * 128 + 128] = both[half * n : half * n + n]
        hb_ref[j, y, c, 0:n] = ho_ref[j, c, 0:n]

    def heads_done(j):
        head_values(j)
        some = pl.ds(0, CHUNK[j])
        target = hb_ref.at[j, y, c, some]
        send(ho_ref.at[j, 1 - c, some], target, d2_s.at[0], d2_r.at[j], c=1 - c)
        for d in (1, -1):
            send(ho_ref.at[j, c, some], target, hy_s.at[0], hy_r.at[j, 0], y=around(y, d))

    def partner_half(j):
        ref = hb_ref.at[j, y, 1 - c, pl.ds(0, CHUNK[j])]
        arrived(ref, d2_r.at[j])
        for d in (1, -1):
            send(ref, ref, hy_s.at[0], hy_r.at[j, 0], y=around(y, d))

    def pass_on(j):
        some = pl.ds(0, CHUNK[j])
        arrived(hb_ref.at[j, pl.ds(0, 2), pl.ds(0, 2), some], hy_r.at[j, 0])
        for k, d in enumerate((1, -1)):
            ref = hb_ref.at[j, around(y, -d), k, some]
            send(ref, ref, hy_s.at[0], hy_r.at[j, 1], y=around(y, d))

    def product(j, zs):
        n = CHUNK[j]
        tokens = jnp.concatenate(
            [hb_ref[j, :, k, 0:n].reshape(4 * n, 1024) for k in range(2)], axis=1
        )
        columns = jnp.concatenate([wo_all[k, zs] for k in range(2)], axis=1)
        ct_ref[j, zs, :, 0 : 4 * n] = nt(columns, tokens).astype(BF)

    def multiply_far(j):
        n = CHUNK[j]
        lanes = pl.ds(0, 4 * n)
        arrived(hb_ref.at[j, around(y, 2), pl.ds(0, 2), pl.ds(0, n)], hy_r.at[j, 1])

        product(j, lax.rem(x + 2, 4))
        for k, d in enumerate((1, -1)):
            send(
                ct_ref.at[j, around(x, 2), pl.ds(k * 224, 224), lanes], r1_ref.at[j, k, :, lanes],
                r1_s.at[0], r1_r.at[j], x=around(x, d),
            )

    def multiply_near(j):
        lanes = pl.ds(0, 4 * CHUNK[j])

        def rest(m, carry):
            product(j, lax.rem(x + jnp.where(m == 0, 1, jnp.where(m == 1, 3, 0)), 4))
            return carry

        lax.fori_loop(0, 3, rest, 0)
        for k, d in enumerate((1, -1)):
            part = pl.ds((1 - k) * 224, 224)
            send(
                ct_ref.at[j, around(x, d), part, lanes], rx_ref.at[j, k, part, lanes], r2_s.at[0],
                r2_r.at[j], x=around(x, d),
            )

    def multiply(j):
        multiply_far(j)
        multiply_near(j)

    def add_far(j):
        n = 4 * CHUNK[j]
        lanes = pl.ds(0, n)
        arrived(r1_ref.at[j, :, :, lanes], r1_r.at[j])
        for k, d in enumerate((1, -1)):
            rows = slice(k * 224, k * 224 + 224)
            near = around(x, d)
            both = ct_ref[j, near, rows, 0:n].astype(F32) + r1_ref[j, k, :, 0:n].astype(F32)
            ct_ref[j, near, rows, 0:n] = both.astype(BF)
            part = pl.ds(k * 224, 224)
            send(
                ct_ref.at[j, near, part, lanes], rx_ref.at[j, k, part, lanes], r2_s.at[0],
                r2_r.at[j], x=near,
            )

    def collect(j):
        n = 4 * CHUNK[j]
        total = (
            ct_ref[j, x, :, 0:n].astype(F32)
            + rx_ref[j, 0, :, 0:n].astype(F32)
            + rx_ref[j, 1, :, 0:n].astype(F32)
        )
        if j % 2 == 0:
            fs_ref[...] = total
            return
        lane = lax.broadcasted_iota(jnp.int32, (448, 128), 1)
        for v in range(2):
            early = fs_ref[:, v * 128 : v * 128 + 128]
            late = total[:, v * 128 : v * 128 + 128]
            at = j // 2 * 4 + 2 * v
            ft_ref[at] = jnp.where(lane < 64, early, pltpu.roll(late, 64, 1)).astype(BF)
            ft_ref[at + 1] = jnp.where(lane < 64, pltpu.roll(early, 64, 1), late).astype(BF)

    here = y // 2 == c

    def add_near(j):
        arrived(rx_ref.at[j, :, :, pl.ds(0, 4 * CHUNK[j])], r2_r.at[j])
        collect(j)
        if j % 2 == 0:
            return
        pair = j // 2
        target = ot_ref.at[
            pl.ds(pl.multiple_of(lax.rem(y, 2) * 448, 448), 448),
            pl.ds(pl.multiple_of((pair * 2 + c) * 128, 128), 128),
        ]
        for d in (2, 1, 3):
            to = around(y, d)
            send(ft_ref.at[pair * 4 + to], target, f_sem.at[0], f_sem.at[1], y=to, c=y // 2)

        @pl.when(here)
        def _():
            target[...] = ft_ref[pair * 4 + y]

        @pl.when(jnp.logical_not(here))
        def _():
            send(ft_ref.at[pair * 4 + y], target, f_sem.at[2], f_sem.at[1], c=1 - c)

    plan = {
        0: [(values_pass, 2)],
        1: [(values_pass, 3)],
        3: [
            (values_ready,), (heads_done, 0), (out_pass,), (project_rest, 0), (partner_half, 0),
            (project_rest, 1),
        ],
        4: [(pass_on, 0)],
        6: [(out_near,)],
        7: [(heads_done, 1)],
        8: [(partner_half, 1)],
        10: [(out_far,)],
        11: [(pass_on, 1), (heads_done, 2), (out_ready,), (multiply, 0)],
        12: [(partner_half, 2)],
        13: [(add_far, 0), (multiply_far, 1)],
        15: [(pass_on, 2), (heads_done, 3)],
        16: [(add_near, 0), (partner_half, 3), (multiply_near, 1), (add_far, 1)],
        17: [(multiply, 2)],
        18: [(pass_on, 3), (add_far, 2), (add_near, 1)],
        19: [(multiply, 3), (add_near, 2), (add_far, 3), (add_near, 3)],
    }

    def run(events):
        for event, *which in events:
            event(*which)

    def together(i, carry):
        two(i)
        for slot in range(16):
            if slot in plan:

                @pl.when(i == slot)
                def _():
                    run(plan[slot])

        return carry

    lax.fori_loop(0, 16, together, 0)
    for slot in range(16, 20):
        run(plan[slot])

    @pl.when(here)
    def _():
        arrived(ft_ref.at[0:6], f_sem.at[1])

    @pl.when(jnp.logical_not(here))
    def _():
        arrived(ft_ref.at[0:8], f_sem.at[1])

    keep_out.start()
    left(packs.at[0:7], a2a_sem.at[0])
    left(opack.at[0:7], o2a_sem.at[0])
    left(ntp.at[0:7], nt_sem.at[0])
    left(ntp.at[0:6], nyz_sem.at[0])
    left(u_ref.at[0:15], ag_s.at[0])
    left(v_ref.at[0:15], uv_s.at[0])
    left(wo_all.at[0, 0:3], oz_sem.at[0])
    left(wo_all.at[0], od_sem.at[0])
    left(ho_ref.at[0:2], d2_s.at[0])
    left(hb_ref.at[0:3], hy_s.at[0])
    left(ct_ref.at[0], r1_s.at[0])
    left(ct_ref.at[0:2], r2_s.at[0])
    left(ft_ref.at[0:6], f_sem.at[0])

    @pl.when(jnp.logical_not(here))
    def _():
        left(ft_ref.at[0:2], f_sem.at[2])

    keep_sel.wait()
    keep_out.wait()


def layer(uq, wk, wv, wo, q, latk, ropk, slot_of, lengths, frequency, cache_latent, cache_rope):
    vmem = pl.BlockSpec(memory_space=pltpu.VMEM)
    smem = pl.BlockSpec(memory_space=pltpu.SMEM)
    hbm = pl.BlockSpec(memory_space=pl.ANY)
    dma = pltpu.SemaphoreType.DMA
    scratch = [
        ((12, 12288), F32), ((4, 8192), F32), ((4, 8192), F32), ((56, 8192), F32),
        ((SEQS, 4, QRANK), BF), ((SEQS, 4, KVRANK), BF), ((2, TOK, TOK), BF), ((TOK, TOK), BF),
        ((TOK, 128), F32), ((TOK, 128), F32),
        ((8, 16, 1792), F32), ((8, 16, 1792), BF), ((8, 16, 1792), BF),
        ((8, 56, 1024), BF), ((8, 56, 1024), BF),
        ((16, 128, 1408), BF), ((16, 32, 1024), BF), ((2, 4, 448, 1024), BF),
        ((3, 8, 128), F32), ((8, 8, 128), F32), ((4, 8, 128), F32), ((4, 8, 128), F32),
        ((TOK, QRANK), BF), ((TOK, KVRANK), BF), ((TOK, ROPE), BF),
        ((HL, TOK, KVRANK), BF), ((HL, TOK, 128), BF), ((HL, TOK, KVRANK), BF),
        ((SLOTS, 4, CACHE, KVRANK), BF), ((SLOTS, 4, ROPE, CACHE), BF),
        ((128, CACHE), F32), ((128, 16), F32), ((128, CACHE), F32), ((128, 16), F32),
        ((4, 2, 64, 1024), BF), ((4, 4, 2, 64, 1024), BF),
        ((4, 4, 448, 256), BF), ((4, 2, 224, 256), BF), ((4, 2, 448, 256), BF),
        ((448, 256), F32), ((8, 448, 128), BF), ((896, TOK), BF),
    ]
    counts = [
        (8,), (SLOTS,), (SLOTS,), (2,), (2,), (2,), (3,), (1,), (25,), (1,), (13,),
        (4,), (2,), (1,), (4,), (1,), (4, 2), (1,), (4,), (1,), (4,), (3,),
    ]
    return pl.pallas_call(
        layer_kernel,
        out_shape=(
            jax.ShapeDtypeStruct((896, TOK), BF), jax.ShapeDtypeStruct((TOK, TOK), BF),
            jax.ShapeDtypeStruct((1,), F32),
        ),
        in_specs=[vmem] * 4 + [smem] + [hbm] * 8,
        out_specs=(hbm, hbm, smem),
        scratch_shapes=[pltpu.VMEM(s, d) for s, d in scratch] + [dma(n) for n in counts],
        compiler_params=pltpu.CompilerParams(
            vmem_limit_bytes=67043328, collective_id=0, has_side_effects=True
        ),
        name="layer",
    )(
        ropk, slot_of, lengths.reshape(1, SEQS), frequency, lengths,
        uq, wk, wv, wo, q, latk, cache_latent, cache_rope,
    )


def shards(q_latent, new_latent, new_rope, cache_latent, cache_rope, lengths, assignment, w_uq, w_uk, w_uv, w_o):
    half = ROPE // 2
    frequency = 10000.0 ** (-np.arange(half, dtype=np.float32) / half)
    frequency = np.broadcast_to(np.tile(frequency, 4)[None, :], (8, 128)).astype(np.float32)
    held, sel, norm = layer(
        w_uq, w_uk, w_uv, w_o.T, q_latent, new_latent, new_rope.transpose(1, 2, 0), assignment,
        lengths, jnp.asarray(frequency), cache_latent, cache_rope,
    )
    out = nt(sel, held).astype(BF).reshape(SEQS, NEWTOK, 896)
    return out, norm


def solution(mesh):
    split = Mesh(mesh.devices.reshape(4, 4, 4, 2), ("dp_0", "dp_1", "tp_0", "tp_1"))
    dp, tp = ("dp_0", "dp_1"), ("tp_0", "tp_1")
    placed = (
        P(dp, None, None), P(dp, None, None), P(dp, None, None), P(dp, None, None), P(dp, None, None),
        P(dp), P(dp, None), P(dp + tp, None), P(dp + tp, None), P(dp + tp, None), P(None, dp + tp),
    )
    return jax.shard_map(
        shards, mesh=split, in_specs=placed, out_specs=(P(dp, None, tp), P()), check_vma=False
    )
```
